32 devices in a mesh: gx: 2 (over x), gy: 4 (over z), gz: 4 (over y, core).
Axes of the slice: x: 2, y: 2, z: 4, core: 2. Of those that a mesh axis runs over, the one named last changes fastest.
Arguments:
- right_side: float32 [16, 64, 512], P('gx', 'gy', 'gz'), may hold values from -40 to 40
- fiber_class: int32 [16, 64, 512], P('gx', 'gy', 'gz'), may hold values from 0 to 15
- conductivity_scale: float32 [16, 64, 512], P('gx', 'gy', 'gz'), may hold values from 0.8 to 1.25
- class_tensor: float32 [6, 16], replicated, may hold values from -0.15 to 1.8, as said below
- block_ids: int32 [2, 4, 8], replicated, may hold values from 0 to 63, as said below
Outputs:
- solution: float32 [16, 64, 512], P('gx', 'gy', 'gz')
- residual: float32 [16, 64, 512], P('gx', 'gy', 'gz')
The draws below stay inside these ranges and needn't reach their ends.
Inputs may be any that keep to these rules, and one draw needn't show every extreme that they name: `class_tensor`: column k is the tensor t I + (l - t) f f^T for a unit vector f, with 1 <= t <= 1.5 and 1.05 <= l / t <= 1.2. `block_ids`: each subdomain number names exactly 1 block.
All inputs are finite; a program needn't handle non-finite values.
Results may differ from the reference program's by a relative error of at most 0.0003.
Values sent between devices are 32-bit elements; how exact they have to be, the bound alone decides.
A program may use at most 64 MiB of HBM per device.

```python
import math
import jax
import jax.numpy as jnp
from jax import lax

CX = 8
CY = 16
BZ = 64
COARSE = 64
NCLS = 16
ITERS = 2
NX = 16
NY = 64
NZ = 512
NBX = 2
NBY = 4
NBZ = 8


def draw_right_side(key, part):
    noise_key, spread_key = jax.random.split(jax.random.fold_in(key, 11))
    shape = (NX, NY, NZ)
    depth = (jnp.arange(NZ, dtype=jnp.float32) + 0.5) / NZ
    ramp = (1.0 + 2.0 * depth)[None, None, :]
    noise = jax.random.truncated_normal(noise_key, -4.0, 4.0, shape, jnp.float32)
    spread = jnp.exp(jax.random.uniform(spread_key, shape, jnp.float32, 0.0, math.log(10.0)))
    return (0.3 * noise * spread * ramp).astype(jnp.float32)


def draw_class_tensor(key, part):
    keys = jax.random.split(jax.random.fold_in(key, 23), 4)
    azimuth = jax.random.uniform(keys[0], (NCLS,), jnp.float32, -math.pi, math.pi)
    elevation = jax.random.uniform(keys[1], (NCLS,), jnp.float32, -0.5 * math.pi, 0.5 * math.pi)
    transverse = jnp.exp(jax.random.uniform(keys[2], (NCLS,), jnp.float32, 0.0, math.log(1.5)))
    anisotropy = jnp.exp(jax.random.uniform(keys[3], (NCLS,), jnp.float32, math.log(1.05), math.log(1.2)))
    excess = transverse * (anisotropy - 1.0)
    fiber_x = jnp.cos(elevation) * jnp.cos(azimuth)
    fiber_y = jnp.cos(elevation) * jnp.sin(azimuth)
    fiber_z = jnp.sin(elevation)
    rows = [transverse + excess * fiber_x * fiber_x, transverse + excess * fiber_y * fiber_y, transverse + excess * fiber_z * fiber_z, excess * fiber_x * fiber_y, excess * fiber_x * fiber_z, excess * fiber_y * fiber_z]
    return jnp.stack(rows).astype(jnp.float32)


def draw_block_ids(key, part):
    order = jax.random.permutation(jax.random.fold_in(key, 37), NBX * NBY * NBZ)
    return (order % COARSE).astype(jnp.int32).reshape(NBX, NBY, NBZ)


def set_ends(array, stream_key, low, largest):
    spot = [jax.random.randint(jax.random.fold_in(stream_key, axis), (), 0, length) for axis, length in enumerate(array.shape)]
    longest = array.shape.index(max(array.shape))
    beside = spot[:longest] + [(spot[longest] + 1) % array.shape[longest]] + spot[longest + 1:]
    return array.at[tuple(spot)].set(low).at[tuple(beside)].set(largest)


def level_of(stream_key, shape, shards, low, top_value):
    def one(dim, shards_of):
        heights = jax.random.uniform(jax.random.fold_in(jax.random.fold_in(stream_key, 6), dim), (shards_of,), jnp.float32, low / len(shards), top_value / len(shards))
        return jnp.repeat(jnp.exp(heights), shape[dim] // shards_of).reshape((-1,) + (1,) * (len(shape) - dim - 1))

    gain = one(*shards[0])
    for cut in shards[1:]:
        gain = gain * one(*cut)
    return gain


def setup_inputs(seed: int = 0) -> dict:
    seeds = jax.random.split(jax.random.key(seed), 6)
    right_side = draw_right_side(jax.random.fold_in(seeds[5], 71), 0)
    fiber_class = set_ends(jax.random.randint(seeds[1], (NX, NY, NZ), 0, NCLS), jax.random.fold_in(seeds[1], 1), 0, NCLS - 1).astype(jnp.int32)
    conductivity_scale = jnp.clip(jnp.exp(math.log(1.25) - 0.4462871 * jax.random.uniform(seeds[2], (NX, NY, NZ), jnp.float32) ** level_of(seeds[2], (NX, NY, NZ), ((0, 2), (1, 4), (2, 4)), -0.2, 0.2)), 0.8, 1.25)
    class_tensor = draw_class_tensor(jax.random.fold_in(seeds[5], 71), 0)
    block_ids = draw_block_ids(jax.random.fold_in(seeds[5], 71), 0)
    return dict(right_side=right_side, fiber_class=fiber_class, conductivity_scale=conductivity_scale, class_tensor=class_tensor, block_ids=block_ids)


STENCIL_TAPS = ((1, 0, 0, 0, 1.0), (-1, 0, 0, 0, 1.0), (0, 1, 0, 1, 1.0), (0, -1, 0, 1, 1.0), (0, 0, 1, 2, 1.0), (0, 0, -1, 2, 1.0), (1, 1, 0, 3, 0.5), (-1, -1, 0, 3, 0.5), (1, -1, 0, 3, -0.5), (-1, 1, 0, 3, -0.5), (1, 0, 1, 4, 0.5), (-1, 0, -1, 4, 0.5), (1, 0, -1, 4, -0.5), (-1, 0, 1, 4, -0.5), (0, 1, 1, 5, 0.5), (0, -1, -1, 5, 0.5), (0, 1, -1, 5, -0.5), (0, -1, 1, 5, -0.5))

def shifted(padded, step_x, step_y, step_z):
    width_x = padded.shape[-3] - 2
    width_y = padded.shape[-2] - 2
    width_z = padded.shape[-1] - 2
    return padded[1 + step_x:1 + step_x + width_x, 1 + step_y:1 + step_y + width_y, 1 + step_z:1 + step_z + width_z]

def edge_weights(tensors, step_x, step_y, step_z, component, factor):
    layer = tensors[component]
    return 0.5 * factor * (shifted(layer, 0, 0, 0) + shifted(layer, step_x, step_y, step_z))

def operate(padded, tensors):
    centre = shifted(padded, 0, 0, 0)
    accumulated = jnp.zeros_like(centre)
    for step_x, step_y, step_z, component, factor in STENCIL_TAPS:
        weight = edge_weights(tensors, step_x, step_y, step_z, component, factor)
        accumulated = accumulated + weight * (centre - shifted(padded, step_x, step_y, step_z))
    return accumulated

def class_onehot(labels, count):
    return (labels[..., None] == jnp.arange(count, dtype=jnp.int32)).astype(jnp.float32)

def reach_onehot(length, offset):
    position = jnp.arange(length, dtype=jnp.int32)
    relative = (position + offset) // length + 1
    return (relative[:, None] == jnp.arange(3, dtype=jnp.int32)[None, :]).astype(jnp.float32)

def centre_mask():
    places = jnp.arange(3, dtype=jnp.int32)
    return (places[:, None, None] == 1) & (places[None, :, None] == 1) & (places[None, None, :] == 1)

def tensor_grid(fiber_class, conductivity_scale, class_tensor):
    return tuple((jnp.pad(class_tensor[component][fiber_class] * conductivity_scale, 1) for component in range(6)))

def coarse_matrix(tensors, block_ids):
    highest = lax.Precision.HIGHEST
    rim_weight = jnp.zeros((NBX, NBY, NBZ, 3, 3, 3), jnp.float32)
    for step_x, step_y, step_z, component, factor in STENCIL_TAPS:
        weight = edge_weights(tensors, step_x, step_y, step_z, component, factor)
        weight = weight.reshape(NBX, CX, NBY, CY, NBZ, BZ)
        rim_weight = rim_weight + jnp.einsum('axbycz,xd,ye,zf->abcdef', weight, reach_onehot(CX, step_x), reach_onehot(CY, step_y), reach_onehot(BZ, step_z), precision=highest)
    rim_weight = jnp.where(centre_mask()[None, None, None], 0.0, rim_weight)
    own_hot = class_onehot(block_ids, COARSE)
    padded_ids = jnp.pad(block_ids, 1, constant_values=-1)
    diagonal_terms = jnp.einsum('abck,abc->k', own_hot, jnp.sum(rim_weight, axis=(3, 4, 5)), precision=highest)
    coupling = jnp.zeros((COARSE, COARSE), jnp.float32)
    for off_x in range(3):
        for off_y in range(3):
            for off_z in range(3):
                if off_x == 1 and off_y == 1 and (off_z == 1):
                    continue
                neighbours = padded_ids[off_x:off_x + NBX, off_y:off_y + NBY, off_z:off_z + NBZ]
                coupling = coupling + jnp.einsum('abck,abc,abcl->kl', own_hot, rim_weight[:, :, :, off_x, off_y, off_z], class_onehot(neighbours, COARSE), precision=highest)
    matrix = jnp.diag(diagonal_terms) - coupling
    return 0.5 * (matrix + matrix.T)

def reference(right_side, fiber_class, conductivity_scale, class_tensor, block_ids):
    highest = lax.Precision.HIGHEST
    tensors = tensor_grid(fiber_class, conductivity_scale, class_tensor)
    coarse = coarse_matrix(tensors, block_ids)
    own_hot = class_onehot(block_ids, COARSE)

    def apply_field(field):
        return operate(jnp.pad(field, 1), tensors)

    def restrict(field):
        block_totals = jnp.sum(field.reshape(NBX, CX, NBY, CY, NBZ, BZ), axis=(1, 3, 5))
        return jnp.einsum('abck,abc->k', own_hot, block_totals, precision=highest)

    def prolong(coarse_values):
        per_block = jnp.einsum('abck,k->abc', own_hot, coarse_values, precision=highest)
        return jnp.broadcast_to(per_block[:, None, :, None, :, None], (NBX, CX, NBY, CY, NBZ, BZ)).reshape(NX, NY, NZ)

    def coarse_solve(field):
        return jnp.linalg.solve(coarse, restrict(field))
    coarse_part = prolong(coarse_solve(right_side))
    residual = right_side - apply_field(coarse_part)
    direction = residual
    norm_now = jnp.sum(residual * residual)
    estimate = jnp.zeros_like(right_side)
    for iteration in range(ITERS):
        product = apply_field(direction)
        image_field = product - apply_field(prolong(coarse_solve(product)))
        step_size = norm_now / jnp.sum(direction * image_field)
        estimate = estimate + step_size * direction
        residual = residual - step_size * image_field
        if iteration + 1 < ITERS:
            norm_next = jnp.sum(residual * residual)
            direction = residual + norm_next / norm_now * direction
            norm_now = norm_next
    solution = coarse_part + estimate - prolong(coarse_solve(apply_field(estimate)))
    return (solution, residual)
```

```python
import functools

import jax
import jax.numpy as jnp
from jax import lax
from jax.experimental import pallas as pl
from jax.experimental.pallas import tpu as pltpu
from jax.sharding import PartitionSpec as P

COARSE = 64
LANES = 128
HIGHEST = lax.Precision.HIGHEST
MESH = pl.DeviceIdType.MESH
F32 = jnp.float32

XX, XZ, XY, YY, YZ, ZZ = range(6)
TABLE_ROW = {XX: 0, YY: 1, ZZ: 2, XY: 3, XZ: 4, YZ: 5}
ZSLOT = {XZ: 0, YZ: 1, ZZ: 2}

TAPS = (
    (1, 0, 0, XX, 0.5),
    (-1, 0, 0, XX, 0.5),
    (0, 1, 0, YY, 0.5),
    (0, -1, 0, YY, 0.5),
    (0, 0, 1, ZZ, 0.5),
    (0, 0, -1, ZZ, 0.5),
    (1, 1, 0, XY, 0.25),
    (-1, -1, 0, XY, 0.25),
    (1, -1, 0, XY, -0.25),
    (-1, 1, 0, XY, -0.25),
    (1, 0, 1, XZ, 0.25),
    (-1, 0, -1, XZ, 0.25),
    (1, 0, -1, XZ, -0.25),
    (-1, 0, 1, XZ, -0.25),
    (0, 1, 1, YZ, 0.25),
    (0, -1, -1, YZ, 0.25),
    (0, 1, -1, YZ, -0.25),
    (0, -1, 1, YZ, -0.25),
)
OFFSETS = tuple(tap[:3] for tap in TAPS)
SLOT = {offset: i for i, offset in enumerate(OFFSETS)}
ZOFFSETS = tuple(o for o in OFFSETS if o[2])
ZINDEX = {offset: i for i, offset in enumerate(ZOFFSETS)}
XYOFFSETS = tuple(o for o in OFFSETS if o[0] and o[1])
XYINDEX = {offset: i for i, offset in enumerate(XYOFFSETS)}
TOP = 8


def neg(offset):
    return tuple(-s for s in offset)


def iota(shape, dim):
    return lax.broadcasted_iota(jnp.int32, shape, dim)


def kernel(
    dims,
    ids_ref,
    table_ref,
    right_ref,
    class_ref,
    scale_ref,
    sol_ref,
    res_ref,
    tens,
    tens_p,
    tens_m,
    weight,
    field,
    field_p,
    field_m,
    prod,
    image,
    rim,
    inverse,
    t_ypack,
    t_yr,
    t_xyr,
    t_zpack,
    t_zr,
    f_ypack,
    f_yr,
    f_xyr,
    f_zpack,
    f_zr,
    msg1,
    gat1,
    den1,
    msg2,
    gat2,
    den2,
    halo_send,
    halo_recv,
    gat_send,
    gat_recv,
):
    nx, ny, nz, bx, by, zblk, nbx, nby, nbz = dims
    bz = LANES
    span = bz // zblk
    count = nx * ny * nz
    px, py, pz = lax.axis_index("gx"), lax.axis_index("gy"), lax.axis_index("gz")
    me = (px * ny + py) * nz + pz
    rows = slice(TOP, TOP + by)
    own = slice(1, 1 + bx)

    tens[0:3, 0, rows, :] = jnp.zeros((3, by, bz), F32)
    tens[0:3, bx + 1, rows, :] = jnp.zeros((3, by, bz), F32)
    for e in range(2):
        field[e, 0, rows, :] = jnp.zeros((by, bz), F32)
        field[e, bx + 1, rows, :] = jnp.zeros((by, bz), F32)
    for buffer in (t_yr, t_xyr, t_zr, f_yr, f_xyr, f_zr):
        buffer[...] = jnp.zeros(buffer.shape, F32)

    def other(d):
        t = lax.rem(me + d, count)
        return (lax.div(t, ny * nz), lax.rem(lax.div(t, nz), ny), lax.rem(t, nz))

    barrier = pltpu.get_barrier_semaphore()

    @pl.loop(1, count)
    def _(d):
        pl.semaphore_signal(barrier, inc=1, device_id=other(d), device_id_type=MESH)

    lane1 = iota((1, bz), 1)
    place = lane1 % span
    block = lane1 // span
    first, last = place == 0, place == span - 1

    def read_id(x, y, z):
        inside = (x >= 0) & (x < nbx) & (y >= 0) & (y < nby) & (z >= 0) & (z < nbz)
        value = ids_ref[
            jnp.clip(x, 0, nbx - 1), jnp.clip(y, 0, nby - 1), jnp.clip(z, 0, nbz - 1)
        ]
        return jnp.where(inside, value, COARSE)

    window = {}
    for dx in range(3):
        for dy in range(3):
            for dz in range(zblk + 2):
                window[dx, dy, dz] = read_id(px + dx - 1, py + dy - 1, pz * zblk + dz - 1)
    around = []
    row48 = iota((48, LANES), 0)
    lane48 = iota((48, LANES), 1)
    for j in range(zblk):
        ids = jnp.full((48, LANES), -1, jnp.int32)
        for dz in range(3):
            for dx in range(3):
                for dy in range(3):
                    ids = jnp.where(
                        row48 == dz * 16 + dx * 3 + dy, window[dx, dy, j + dz], ids
                    )
        around.append((ids == lane48).astype(F32))
    own_id = [window[1, 1, j + 1] for j in range(zblk)]

    for x in range(bx):
        kind = class_ref[x]
        parts = [jnp.full((by, bz), table_ref[c, 0], F32) for c in range(6)]
        for k in range(1, table_ref.shape[1]):
            match = kind == k
            parts = [jnp.where(match, table_ref[c, k], parts[c]) for c in range(6)]
        for slot in range(6):
            tens[slot, 1 + x, rows, :] = parts[TABLE_ROW[slot]] * scale_ref[x]

    def own_tensor(slot):
        return tens[slot, own, rows, :]

    def halves(row):
        return [
            jnp.sum(jnp.where(block == j, row, 0.0), axis=1, keepdims=True) for j in range(zblk)
        ]

    def plane_sum(slot, x):
        return jnp.sum(tens[slot, 1 + x, rows, :], axis=0, keepdims=True)

    def line_sum(slot, y):
        total = tens[slot, 1, TOP + y : TOP + y + 1, :]
        for x in range(1, bx):
            total = total + tens[slot, 1 + x, TOP + y : TOP + y + 1, :]
        return total

    def corner(x, y):
        return tens[XY, 1 + x, TOP + y : TOP + y + 1, :]

    hi_x, hi_y = bx - 1, by - 1
    c00, c01, c10, c11 = corner(0, 0), corner(0, hi_y), corner(hi_x, 0), corner(hi_x, hi_y)
    xz_lo, xz_hi = plane_sum(XZ, 0), plane_sum(XZ, hi_x)
    yz_lo, yz_hi = line_sum(YZ, 0), line_sum(YZ, hi_y)
    zz_all = jnp.sum(jnp.sum(own_tensor(ZZ), axis=0), axis=0, keepdims=True)
    flat = {
        (1, 0): 0.5 * plane_sum(XX, hi_x) + 0.25 * (c10 - c11),
        (-1, 0): 0.5 * plane_sum(XX, 0) + 0.25 * (c01 - c00),
        (0, 1): 0.5 * line_sum(YY, hi_y) + 0.25 * (c01 - c11),
        (0, -1): 0.5 * line_sum(YY, 0) + 0.25 * (c10 - c00),
        (1, 1): 0.25 * c11,
        (-1, -1): 0.25 * c00,
        (1, -1): -0.25 * c10,
        (-1, 1): -0.25 * c01,
    }
    tilted = {
        (1, 0): 0.25 * xz_hi,
        (-1, 0): -0.25 * xz_lo,
        (0, 1): 0.25 * yz_hi,
        (0, -1): -0.25 * yz_lo,
    }
    slant = 0.25 * (xz_lo - xz_hi + yz_lo - yz_hi)
    rim[...] = jnp.zeros(rim.shape, F32)
    for key, row in flat.items():
        at = (key[0] + 1) * 3 + key[1] + 1
        if key in tilted:
            up = jnp.where(last, tilted[key], 0.0)
            down = jnp.where(first, -tilted[key], 0.0)
            rim[at : at + 1, :] = down
            rim[32 + at : 33 + at, :] = up
            row = row - up - down
        rim[16 + at : 17 + at, :] = row
    rim[4:5, :] = jnp.where(first, 0.5 * zz_all - slant, 0.0)
    rim[36:37, :] = jnp.where(last, 0.5 * zz_all + slant, 0.0)

    sums = jnp.sum(jnp.sum(right_ref[...], axis=0), axis=0, keepdims=True)
    totals = halves(sums)
    block48 = lane48 // span
    for j in range(zblk):
        leaving = jnp.sum(jnp.where(block48 == j, rim[...], 0.0), axis=1, keepdims=True)
        row = jnp.sum(leaving * around[j], axis=0, keepdims=True)
        row = jnp.where(lane1 == COARSE + 1, totals[j], row)
        row = jnp.where(lane1 == COARSE + 2, own_id[j].astype(F32), row)
        msg1[j : j + 1, :] = row
        gat1[me, j : j + 1, :] = row

    lane8, row8 = iota((8, LANES), 1), iota((8, LANES), 0)

    def pick(i):
        return (
            ((row8 == i) & (lane8 == 0)) | ((row8 == i + 3) & (lane8 == bz - 1))
        ).astype(F32)

    def faces(cells, i):
        return lax.dot_general(
            pick(i),
            cells.reshape(bx * by, bz),
            (((1,), (1,)), ((), ())),
            precision=HIGHEST,
            preferred_element_type=F32,
        )

    t_zpack[...] = (
        faces(own_tensor(XZ), 0) + faces(own_tensor(YZ), 1) + faces(own_tensor(ZZ), 2)
    )
    for side, y in ((0, 0), (1, hi_y)):
        for i, slot in enumerate((XY, YY, YZ)):
            for x in range(bx):
                t_ypack[side, i, x : x + 1, :] = tens[slot, 1 + x, TOP + y : TOP + y + 1, :]

    pl.semaphore_wait(barrier, count - 1)

    def spread(msg, gat, g):
        @pl.loop(1, count)
        def _(d):
            pltpu.make_async_remote_copy(
                src_ref=msg,
                dst_ref=gat.at[me],
                send_sem=gat_send.at[g],
                recv_sem=gat_recv.at[g],
                device_id=other(d),
                device_id_type=MESH,
            ).start()

    def gathered(gat, g):
        every = pltpu.make_async_remote_copy(
            src_ref=gat.at[pl.ds(0, count - 1)],
            dst_ref=gat.at[pl.ds(0, count - 1)],
            send_sem=gat_send.at[g],
            recv_sem=gat_recv.at[g],
            device_id=other(1),
            device_id_type=MESH,
        )
        every.wait_send()
        every.wait_recv()

    def exchange(e, ends):
        def copies():
            for offset in OFFSETS:
                dx, dy, dz = offset
                tx, ty, tz = px + dx, py + dy, pz + dz
                inside = None
                for step, at, size in ((dx, tx, nx), (dy, ty, ny), (dz, tz, nz)):
                    if step:
                        ok = (at < size) if step > 0 else (at >= 0)
                        inside = ok if inside is None else inside & ok
                source, target = ends(offset)
                yield inside, pltpu.make_async_remote_copy(
                    src_ref=source,
                    dst_ref=target,
                    send_sem=halo_send.at[e, SLOT[offset]],
                    recv_sem=halo_recv.at[e, SLOT[neg(offset)]],
                    device_id=(tx, ty, tz),
                    device_id_type=MESH,
                )

        def landings():
            for offset in OFFSETS:
                dx, dy, dz = offset
                tx, ty, tz = px + dx, py + dy, pz + dz
                inside = None
                for step, at, size in ((dx, tx, nx), (dy, ty, ny), (dz, tz, nz)):
                    if step:
                        ok = (at < size) if step > 0 else (at >= 0)
                        inside = ok if inside is None else inside & ok
                source, target = ends(neg(offset))
                yield inside, pltpu.make_async_remote_copy(
                    src_ref=source,
                    dst_ref=target,
                    send_sem=halo_send.at[e, SLOT[offset]],
                    recv_sem=halo_recv.at[e, SLOT[offset]],
                    device_id=(tx, ty, tz),
                    device_id_type=MESH,
                )

        def begin():
            for inside, copy in copies():
                pl.when(inside)(copy.start)

        def finish():
            for inside, copy in landings():
                pl.when(inside)(copy.wait_recv)
            for inside, copy in copies():
                pl.when(inside)(copy.wait_send)

        return begin, finish

    def tensor_ends(offset):
        dx, dy, dz = offset
        if dz:
            return t_zpack, t_zr.at[ZINDEX[neg(offset)]]
        if dx and dy:
            return t_ypack.at[(dy + 1) // 2, 0], t_xyr.at[XYINDEX[neg(offset)]]
        if dx:
            source, target = (bx, 0) if dx > 0 else (1, bx + 1)
            return tens.at[pl.ds(0, 3), source, pl.ds(TOP, by)], tens.at[
                pl.ds(0, 3), target, pl.ds(TOP, by)
            ]
        return t_ypack.at[(dy + 1) // 2], t_yr.at[(1 - dy) // 2]

    def field_ends(e):
        def ends(offset):
            dx, dy, dz = offset
            if dz:
                return f_zpack.at[e], f_zr.at[e, ZINDEX[neg(offset)]]
            if dx and dy:
                return f_ypack.at[e, (dy + 1) // 2], f_xyr.at[e, XYINDEX[neg(offset)]]
            if dx:
                source, target = (bx, 0) if dx > 0 else (1, bx + 1)
                return field.at[e, source, pl.ds(TOP, by)], field.at[e, target, pl.ds(TOP, by)]
            return f_ypack.at[e, (dy + 1) // 2], f_yr.at[e, (1 - dy) // 2]

        return ends

    spread(msg1, gat1, 0)
    begin, finish = exchange(0, tensor_ends)
    begin()
    finish()

    def corners_in(buffer, arrived):
        for offset in XYOFFSETS:
            dx, dy, _ = offset
            x = bx + 1 if dx > 0 else 0
            y = TOP + by if dy > 0 else TOP - 1
            row = 0 if dx > 0 else hi_x
            buffer[x, y : y + 1, :] = arrived[XYINDEX[offset], row : row + 1, :]

    def lines_in(buffer, arrived, side):
        y = TOP - 1 if side == 0 else TOP + by
        for x in range(bx):
            buffer[1 + x, y : y + 1, :] = arrived[x : x + 1, :]

    def shifted(cells, dz, column):
        turned = pltpu.roll(cells, bz - 1 if dz > 0 else 1, 1)
        edge = bz - 1 if dz > 0 else 0
        return jnp.where(iota(cells.shape, 1) == edge, column, turned)

    def tilt(centre, up, down, arrived, i, lines, with_x, with_y):
        stack = []
        for dz in (1, -1):
            r = i if dz > 0 else i + 3

            def row_of(offset):
                return arrived[ZINDEX[offset], r : r + 1, :]

            stack.append(row_of((0, 0, dz)))
            stack.append(
                jnp.where(lane1 < by, row_of((1, 0, dz)), row_of((-1, 0, dz)))
                if with_x
                else jnp.zeros((1, bz), F32)
            )
            stack.append(
                jnp.where(lane1 % by == 0, row_of((0, 1, dz)), row_of((0, -1, dz)))
                if with_y
                else jnp.zeros((1, bz), F32)
            )
        stack = stack + [jnp.zeros((2, bz), F32)]
        columns = jnp.concatenate(stack, axis=0).T
        cells = centre[own, rows, :].reshape(bx * by, bz)
        for dz, out, k in ((1, up, 0), (-1, down, 3)):
            moved = shifted(cells, dz, columns[:, k : k + 1])
            out[own, rows, :] = moved.reshape(bx, by, bz)
            if with_x:
                out[0, rows, :] = shifted(
                    centre[0, rows, :], dz, columns[hi_x * by : bx * by, k + 1 : k + 2]
                )
                out[bx + 1, rows, :] = shifted(
                    centre[bx + 1, rows, :], dz, columns[0:by, k + 1 : k + 2]
                )
            if with_y:
                for side, at, inner in ((0, TOP - 1, hi_y), (1, TOP + by, 0)):
                    edge = jnp.concatenate(
                        [
                            columns[x * by + inner : x * by + inner + 1, k + 2 : k + 3]
                            for x in range(bx)
                        ],
                        axis=0,
                    )
                    moved = shifted(lines[side], dz, edge)
                    for x in range(bx):
                        out[1 + x, at : at + 1, :] = moved[x : x + 1, :]

    for side in range(2):
        for i, slot in enumerate((XY, YY, YZ)):
            lines_in(tens.at[slot], t_yr.at[side, i], side)
    corners_in(tens.at[XY], t_xyr)
    for slot, with_x, with_y in ((XZ, True, False), (YZ, False, True), (ZZ, False, False)):
        i = ZSLOT[slot]
        tilt(
            tens.at[slot],
            tens_p.at[i],
            tens_m.at[i],
            t_zr,
            i,
            (t_yr[0, 2], t_yr[1, 2]),
            with_x,
            with_y,
        )

    for t, (dx, dy, dz, slot, factor) in enumerate(TAPS):
        for x in range(bx):
            here = tens[slot, 1 + x, rows, :]
            there_rows = slice(TOP + dy, TOP + dy + by)
            if dz:
                beside = tens_p if dz > 0 else tens_m
                there = beside[ZSLOT[slot], 1 + x + dx, there_rows, :]
            else:
                there = tens[slot, 1 + x + dx, there_rows, :]
            weight[t, x] = factor * (here + there)

    gathered(gat1, 0)
    for d in range(count):
        den1[d * zblk : (d + 1) * zblk, :] = gat1[d]
    every = den1[...]
    lane_b = iota(every.shape, 1)
    number = every[:, COARSE + 2 : COARSE + 3]
    hot = (lane_b.astype(F32) == number).astype(F32)
    rhs = jnp.sum(every[:, COARSE + 1 : COARSE + 2] * hot, axis=0, keepdims=True)
    parts = jnp.where(lane_b <= COARSE, every, 0.0)
    flow = lax.dot_general(
        hot, parts, (((0,), (0,)), ((), ())), precision=HIGHEST, preferred_element_type=F32
    )
    back = lax.dot_general(
        parts, hot, (((0,), (0,)), ((), ())), precision=HIGHEST, preferred_element_type=F32
    )
    flow, back = flow[0:COARSE], back[0:COARSE]
    row_c, lane_c = iota((COARSE, LANES), 0), iota((COARSE, LANES), 1)
    outward = jnp.sum(flow, axis=1, keepdims=True)
    inward = jnp.sum(flow, axis=0, keepdims=True)
    coarse = jnp.where(row_c == lane_c, outward + inward, 0.0) - flow - back
    work = jnp.where(
        lane_c < COARSE,
        (row_c == lane_c).astype(F32),
        pltpu.roll(jnp.where(lane_c < COARSE, coarse, 0.0), COARSE, 1),
    )
    for k in range(COARSE):
        column = jnp.broadcast_to(work[:, COARSE + k : COARSE + k + 1], (COARSE, LANES))
        row = work[k : k + 1, :] / column[k : k + 1, :]
        work = jnp.where(row_c == k, row, work - column * row)
    inverse[0:COARSE, :] = jnp.where(lane_c < COARSE, work, 0.0)
    inverse[COARSE:LANES, :] = jnp.zeros((LANES - COARSE, LANES), F32)

    def solve(row):
        wide = jnp.broadcast_to(row, (8, LANES))
        got = jnp.dot(wide, inverse[...], precision=HIGHEST, preferred_element_type=F32)
        return got[0:1]

    row16, lane16 = iota((16, LANES), 0), iota((16, LANES), 1)
    place16, block16 = lane16 % span, lane16 // span

    def steps(values):
        flat_rows = jnp.zeros((16, LANES), F32)
        up_rows, down_rows = flat_rows, flat_rows
        for j in range(zblk):
            u = jnp.sum(around[j] * values, axis=1, keepdims=True)
            mine = block16 == j
            flat_rows = jnp.where(mine, u[16:32], flat_rows)
            up_rows = jnp.where(mine, jnp.where(place16 == span - 1, u[32:48], u[16:32]), up_rows)
            down_rows = jnp.where(mine, jnp.where(place16 == 0, u[0:16], u[16:32]), down_rows)
        centre = flat_rows[4:5]
        return centre, {0: centre - flat_rows, 1: centre - up_rows, -1: centre - down_rows}

    plane_row = iota((by, bz), 0)

    def coarse_image(diffs, x):
        total = jnp.zeros((by, bz), F32)
        for t, (dx, dy, dz, _, _) in enumerate(TAPS):
            ax = 1 if x + dx >= bx else (-1 if x + dx < 0 else 0)

            def line(ay):
                r = (ax + 1) * 3 + ay + 1
                return diffs[dz][r : r + 1]

            if dz == 0 and ax == 0 and dy == 0:
                continue
            if dy == 0:
                delta = jnp.broadcast_to(line(0), (by, bz))
            else:
                delta = jnp.where(
                    plane_row == (hi_y if dy > 0 else 0), line(dy), line(0)
                )
            total = total + weight[t, x] * delta
        return total

    def begin_field(e):
        cells = field[e, own, rows, :]
        f_zpack[e] = faces(cells, 0)
        for side, y in ((0, 0), (1, hi_y)):
            for x in range(bx):
                f_ypack[e, side, x : x + 1, :] = field[e, 1 + x, TOP + y : TOP + y + 1, :]
        begin, finish = exchange(1 + e, field_ends(e))
        begin()
        return finish

    def operate(e):
        base = field.at[e]
        for side in range(2):
            lines_in(base, f_yr.at[e, side], side)
        corners_in(base, f_xyr.at[e])
        tilt(
            base, field_p, field_m, f_zr.at[e], 0, (f_yr[e, 0], f_yr[e, 1]), True, True
        )
        norm = jnp.zeros((by, bz), F32)
        cross, total = norm, norm
        for x in range(bx):
            here = base[1 + x, rows, :]
            acc = jnp.zeros((by, bz), F32)
            for t, (dx, dy, dz, _, _) in enumerate(TAPS):
                source = base if dz == 0 else (field_p if dz > 0 else field_m)
                there = source[1 + x + dx, TOP + dy : TOP + dy + by, :]
                acc = acc + weight[t, x] * (here - there)
            prod[x] = acc
            norm = norm + here * here
            cross = cross + here * acc
            total = total + acc
        sums = halves(jnp.sum(total, axis=0, keepdims=True))
        row = jnp.zeros((1, LANES), F32)
        for j in range(zblk):
            row = row + jnp.where(lane1 == own_id[j], sums[j], 0.0)
        row = jnp.where(lane1 == COARSE, jnp.sum(norm), row)
        row = jnp.where(lane1 == COARSE + 1, jnp.sum(cross), row)
        msg2[e] = row
        gat2[e, me] = row
        spread(msg2.at[e], gat2.at[e], 1 + e)

    def collect(e):
        gathered(gat2.at[e], 1 + e)
        for d in range(count):
            den2[d : d + 1, :] = gat2[e, d]
        row = jnp.sum(den2[...], axis=0, keepdims=True)
        values = solve(row)
        shared = jnp.sum(row * values, axis=1, keepdims=True)
        norm = row[:, COARSE : COARSE + 1]
        cross = row[:, COARSE + 1 : COARSE + 2] - shared
        return values, norm, cross

    values0 = solve(rhs)
    centre0, diffs = steps(values0)
    for x in range(bx):
        field[0, 1 + x, rows, :] = right_ref[x] - coarse_image(diffs, x)
    finish = begin_field(0)
    finish()
    operate(0)
    values1, norm0, curve0 = collect(0)
    centre1, diffs = steps(values1)
    alpha0 = norm0 / curve0
    for x in range(bx):
        moved = prod[x] - coarse_image(diffs, x)
        image[x] = moved
        field[1, 1 + x, rows, :] = field[0, 1 + x, rows, :] - alpha0 * moved
    finish = begin_field(1)
    finish()
    operate(1)
    values2, norm1, curve1 = collect(1)
    centre2, diffs = steps(values2)
    beta = norm1 / norm0
    alpha1 = norm1 / (curve1 - beta * norm1 / alpha0)
    both = alpha0 + alpha1 * beta
    coarse_row = centre0 - both * centre1 - alpha1 * centre2
    for x in range(bx):
        moved = prod[x] - coarse_image(diffs, x) + beta * image[x]
        now = field[1, 1 + x, rows, :]
        res_ref[x] = now - alpha1 * moved
        sol_ref[x] = coarse_row + both * field[0, 1 + x, rows, :] + alpha1 * now


def solution(mesh):
    nx, ny, nz = (mesh.shape[name] for name in ("gx", "gy", "gz"))
    count = nx * ny * nz

    def body(right_side, fiber_class, conductivity_scale, class_tensor, block_ids):
        bx, by, bz = right_side.shape
        nbx, nby, nbz = block_ids.shape
        zblk = nbz // nz
        dims = (nx, ny, nz, bx, by, zblk, nbx, nby, nbz)
        px, py = bx + 2, by + 16
        vmem = lambda *shape: pltpu.VMEM(shape, F32)
        whole = pl.BlockSpec(memory_space=pltpu.VMEM)
        scalar = pl.BlockSpec(memory_space=pltpu.SMEM)
        return pl.pallas_call(
            functools.partial(kernel, dims),
            out_shape=[jax.ShapeDtypeStruct((bx, by, bz), F32)] * 2,
            in_specs=[scalar, scalar, whole, whole, whole],
            out_specs=[whole, whole],
            scratch_shapes=[
                vmem(6, px, py, bz),
                vmem(3, px, py, bz),
                vmem(3, px, py, bz),
                vmem(18, bx, by, bz),
                vmem(2, px, py, bz),
                vmem(px, py, bz),
                vmem(px, py, bz),
                vmem(bx, by, bz),
                vmem(bx, by, bz),
                vmem(48, bz),
                vmem(LANES, LANES),
                vmem(2, 3, bx, bz),
                vmem(2, 3, bx, bz),
                vmem(4, bx, bz),
                vmem(8, bz),
                vmem(len(ZOFFSETS), 8, bz),
                vmem(2, 2, bx, bz),
                vmem(2, 2, bx, bz),
                vmem(2, 4, bx, bz),
                vmem(2, 8, bz),
                vmem(2, len(ZOFFSETS), 8, bz),
                vmem(zblk, LANES),
                vmem(count, zblk, LANES),
                vmem(count * zblk, LANES),
                vmem(2, 1, LANES),
                vmem(2, count, 1, LANES),
                vmem(count, LANES),
                pltpu.SemaphoreType.DMA((3, 18)),
                pltpu.SemaphoreType.DMA((3, 18)),
                pltpu.SemaphoreType.DMA((3,)),
                pltpu.SemaphoreType.DMA((3,)),
            ],
            compiler_params=pltpu.CompilerParams(collective_id=0, has_side_effects=True),
        )(block_ids, class_tensor, right_side, fiber_class, conductivity_scale)

    placed = (P("gx", "gy", "gz"), P("gx", "gy", "gz"), P("gx", "gy", "gz"), P(), P())
    return jax.shard_map(
        body,
        mesh=mesh,
        in_specs=placed,
        out_specs=(P("gx", "gy", "gz"), P("gx", "gy", "gz")),
        check_vma=False,
    )
```

```python
import functools

import jax
import jax.numpy as jnp
from jax import lax
from jax.experimental import pallas as pl
from jax.experimental.pallas import tpu as pltpu
from jax.sharding import PartitionSpec as P

COARSE = 64
PIVOTS = 4
LANES = 128
HIGHEST = lax.Precision.HIGHEST
MESH = pl.DeviceIdType.MESH
F32 = jnp.float32

XX, XZ, XY, YY, YZ, ZZ = range(6)
TABLE_ROW = {XX: 0, YY: 1, ZZ: 2, XY: 3, XZ: 4, YZ: 5}
ZSLOT = {XZ: 0, YZ: 1, ZZ: 2}

TAPS = (
    (1, 0, 0, XX, 0.5),
    (-1, 0, 0, XX, 0.5),
    (0, 1, 0, YY, 0.5),
    (0, -1, 0, YY, 0.5),
    (0, 0, 1, ZZ, 0.5),
    (0, 0, -1, ZZ, 0.5),
    (1, 1, 0, XY, 0.25),
    (-1, -1, 0, XY, 0.25),
    (1, -1, 0, XY, -0.25),
    (-1, 1, 0, XY, -0.25),
    (1, 0, 1, XZ, 0.25),
    (-1, 0, -1, XZ, 0.25),
    (1, 0, -1, XZ, -0.25),
    (-1, 0, 1, XZ, -0.25),
    (0, 1, 1, YZ, 0.25),
    (0, -1, -1, YZ, 0.25),
    (0, 1, -1, YZ, -0.25),
    (0, -1, 1, YZ, -0.25),
)
OFFSETS = tuple(tap[:3] for tap in TAPS)
SLOT = {offset: i for i, offset in enumerate(OFFSETS)}
ZOFFSETS = tuple(o for o in OFFSETS if o[2])
ZINDEX = {offset: i for i, offset in enumerate(ZOFFSETS)}
XYOFFSETS = tuple(o for o in OFFSETS if o[0] and o[1])
XYINDEX = {offset: i for i, offset in enumerate(XYOFFSETS)}
TOP = 8


def neg(offset):
    return tuple(-s for s in offset)


def iota(shape, dim):
    return lax.broadcasted_iota(jnp.int32, shape, dim)


def kernel(
    dims,
    ids_ref,
    table_ref,
    right_ref,
    class_ref,
    scale_ref,
    sol_ref,
    res_ref,
    tens,
    tens_p,
    tens_m,
    weight,
    field,
    field_p,
    field_m,
    prod,
    image,
    rim,
    inverse,
    t_ypack,
    t_yr,
    t_xyr,
    t_zpack,
    t_zr,
    f_ypack,
    f_yr,
    f_xyr,
    f_zpack,
    f_zr,
    msg1,
    gat1,
    den1,
    msg2,
    gat2,
    halo_send,
    halo_recv,
    gat_send,
    gat_recv,
):
    nx, ny, nz, bx, by, zblk, nbx, nby, nbz = dims
    bz = LANES
    span = bz // zblk
    count = nx * ny * nz
    px, py, pz = lax.axis_index("gx"), lax.axis_index("gy"), lax.axis_index("gz")
    me = (px * ny + py) * nz + pz
    rows = slice(TOP, TOP + by)
    own = slice(1, 1 + bx)

    tens[0:3, 0, rows, :] = jnp.zeros((3, by, bz), F32)
    tens[0:3, bx + 1, rows, :] = jnp.zeros((3, by, bz), F32)
    for e in range(2):
        field[e, 0, rows, :] = jnp.zeros((by, bz), F32)
        field[e, bx + 1, rows, :] = jnp.zeros((by, bz), F32)
    for buffer in (t_yr, t_xyr, t_zr, f_yr, f_xyr, f_zr):
        buffer[...] = jnp.zeros(buffer.shape, F32)

    def other(d):
        t = lax.rem(me + d, count)
        return (lax.div(t, ny * nz), lax.rem(lax.div(t, nz), ny), lax.rem(t, nz))

    steps_far = sorted(
        (
            (dx, dy, dz)
            for dx in range(nx)
            for dy in range(ny)
            for dz in range(nz)
            if dx or dy or dz
        ),
        key=lambda o: -sum(min(d, n - d) for d, n in zip(o, (nx, ny, nz // 2))),
    )

    def each_peer(action):
        if count > 64:
            pl.loop(1, count)(lambda d: action(other(d)))
            return

        def turned(at, n):
            return [at] + [
                jnp.where(at + d >= n, at + d - n, at + d) for d in range(1, n)
            ]

        xs, ys, zs = turned(px, nx), turned(py, ny), turned(pz, nz)
        for dx, dy, dz in steps_far:
            action((xs[dx], ys[dy], zs[dz]))

    barrier = pltpu.get_barrier_semaphore()

    def greet(peer):
        pl.semaphore_signal(barrier, inc=1, device_id=peer, device_id_type=MESH)

    each_peer(greet)

    lane1 = iota((1, bz), 1)
    place = lane1 % span
    block = lane1 // span
    first, last = place == 0, place == span - 1

    def read_id(x, y, z):
        inside = (x >= 0) & (x < nbx) & (y >= 0) & (y < nby) & (z >= 0) & (z < nbz)
        value = ids_ref[
            jnp.clip(x, 0, nbx - 1), jnp.clip(y, 0, nby - 1), jnp.clip(z, 0, nbz - 1)
        ]
        return jnp.where(inside, value, COARSE)

    window = {}
    for dx in range(3):
        for dy in range(3):
            for dz in range(zblk + 2):
                window[dx, dy, dz] = read_id(px + dx - 1, py + dy - 1, pz * zblk + dz - 1)
    around = []
    row48 = iota((48, LANES), 0)
    lane48 = iota((48, LANES), 1)
    for j in range(zblk):
        ids = jnp.full((48, LANES), -1, jnp.int32)
        for dz in range(3):
            for dx in range(3):
                for dy in range(3):
                    ids = jnp.where(
                        row48 == dz * 16 + dx * 3 + dy, window[dx, dy, j + dz], ids
                    )
        around.append((ids == lane48).astype(F32))
    own_id = [window[1, 1, j + 1] for j in range(zblk)]

    for x in range(bx):
        kind = class_ref[x]
        parts = [jnp.full((by, bz), table_ref[c, 0], F32) for c in range(6)]
        for k in range(1, table_ref.shape[1]):
            match = kind == k
            parts = [jnp.where(match, table_ref[c, k], parts[c]) for c in range(6)]
        for slot in range(6):
            tens[slot, 1 + x, rows, :] = parts[TABLE_ROW[slot]] * scale_ref[x]

    def own_tensor(slot):
        return tens[slot, own, rows, :]

    def halves(row):
        return [
            jnp.sum(jnp.where(block == j, row, 0.0), axis=1, keepdims=True) for j in range(zblk)
        ]

    def plane_sum(slot, x):
        return jnp.sum(tens[slot, 1 + x, rows, :], axis=0, keepdims=True)

    def line_sum(slot, y):
        total = tens[slot, 1, TOP + y : TOP + y + 1, :]
        for x in range(1, bx):
            total = total + tens[slot, 1 + x, TOP + y : TOP + y + 1, :]
        return total

    def corner(x, y):
        return tens[XY, 1 + x, TOP + y : TOP + y + 1, :]

    hi_x, hi_y = bx - 1, by - 1
    c00, c01, c10, c11 = corner(0, 0), corner(0, hi_y), corner(hi_x, 0), corner(hi_x, hi_y)
    xz_lo, xz_hi = plane_sum(XZ, 0), plane_sum(XZ, hi_x)
    yz_lo, yz_hi = line_sum(YZ, 0), line_sum(YZ, hi_y)
    zz_all = jnp.sum(jnp.sum(own_tensor(ZZ), axis=0), axis=0, keepdims=True)
    flat = {
        (1, 0): 0.5 * plane_sum(XX, hi_x) + 0.25 * (c10 - c11),
        (-1, 0): 0.5 * plane_sum(XX, 0) + 0.25 * (c01 - c00),
        (0, 1): 0.5 * line_sum(YY, hi_y) + 0.25 * (c01 - c11),
        (0, -1): 0.5 * line_sum(YY, 0) + 0.25 * (c10 - c00),
        (1, 1): 0.25 * c11,
        (-1, -1): 0.25 * c00,
        (1, -1): -0.25 * c10,
        (-1, 1): -0.25 * c01,
    }
    tilted = {
        (1, 0): 0.25 * xz_hi,
        (-1, 0): -0.25 * xz_lo,
        (0, 1): 0.25 * yz_hi,
        (0, -1): -0.25 * yz_lo,
    }
    slant = 0.25 * (xz_lo - xz_hi + yz_lo - yz_hi)
    rim[...] = jnp.zeros(rim.shape, F32)
    for key, row in flat.items():
        at = (key[0] + 1) * 3 + key[1] + 1
        if key in tilted:
            up = jnp.where(last, tilted[key], 0.0)
            down = jnp.where(first, -tilted[key], 0.0)
            rim[at : at + 1, :] = down
            rim[32 + at : 33 + at, :] = up
            row = row - up - down
        rim[16 + at : 17 + at, :] = row
    rim[4:5, :] = jnp.where(first, 0.5 * zz_all - slant, 0.0)
    rim[36:37, :] = jnp.where(last, 0.5 * zz_all + slant, 0.0)

    sums = jnp.sum(jnp.sum(right_ref[...], axis=0), axis=0, keepdims=True)
    totals = halves(sums)
    block48 = lane48 // span
    for j in range(zblk):
        leaving = jnp.sum(jnp.where(block48 == j, rim[...], 0.0), axis=1, keepdims=True)
        row = jnp.sum(leaving * around[j], axis=0, keepdims=True)
        row = jnp.where(lane1 == COARSE + 1, totals[j], row)
        row = jnp.where(lane1 == COARSE + 2, own_id[j].astype(F32), row)
        msg1[j : j + 1, :] = row
        gat1[me, j : j + 1, :] = row

    lane8, row8 = iota((8, LANES), 1), iota((8, LANES), 0)

    def pick(i):
        return (
            ((row8 == i) & (lane8 == 0)) | ((row8 == i + 3) & (lane8 == bz - 1))
        ).astype(F32)

    def faces(cells, i):
        return lax.dot_general(
            pick(i),
            cells.reshape(bx * by, bz),
            (((1,), (1,)), ((), ())),
            precision=HIGHEST,
            preferred_element_type=F32,
        )

    t_zpack[...] = (
        faces(own_tensor(XZ), 0) + faces(own_tensor(YZ), 1) + faces(own_tensor(ZZ), 2)
    )
    for side, y in ((0, 0), (1, hi_y)):
        for i, slot in enumerate((XY, YY, YZ)):
            for x in range(bx):
                t_ypack[side, i, x : x + 1, :] = tens[slot, 1 + x, TOP + y : TOP + y + 1, :]

    pl.semaphore_wait(barrier, count - 1)

    later = []

    def spread(msg, gat, g):
        def send(peer):
            pltpu.make_async_remote_copy(
                src_ref=msg,
                dst_ref=gat.at[me],
                send_sem=gat_send.at[g],
                recv_sem=gat_recv.at[g],
                device_id=peer,
                device_id_type=MESH,
            ).start()

        each_peer(send)

    def gathered(gat, g):
        every = pltpu.make_async_remote_copy(
            src_ref=gat.at[pl.ds(0, count - 1)],
            dst_ref=gat.at[pl.ds(0, count - 1)],
            send_sem=gat_send.at[g],
            recv_sem=gat_recv.at[g],
            device_id=other(1),
            device_id_type=MESH,
        )
        every.wait_recv()
        later.append(every.wait_send)

    def exchange(e, ends):
        def copies():
            for offset in OFFSETS:
                dx, dy, dz = offset
                tx, ty, tz = px + dx, py + dy, pz + dz
                inside = None
                for step, at, size in ((dx, tx, nx), (dy, ty, ny), (dz, tz, nz)):
                    if step:
                        ok = (at < size) if step > 0 else (at >= 0)
                        inside = ok if inside is None else inside & ok
                source, target = ends(offset)
                yield inside, pltpu.make_async_remote_copy(
                    src_ref=source,
                    dst_ref=target,
                    send_sem=halo_send.at[e, SLOT[offset]],
                    recv_sem=halo_recv.at[e, SLOT[neg(offset)]],
                    device_id=(tx, ty, tz),
                    device_id_type=MESH,
                )

        def landings():
            for offset in OFFSETS:
                dx, dy, dz = offset
                tx, ty, tz = px + dx, py + dy, pz + dz
                inside = None
                for step, at, size in ((dx, tx, nx), (dy, ty, ny), (dz, tz, nz)):
                    if step:
                        ok = (at < size) if step > 0 else (at >= 0)
                        inside = ok if inside is None else inside & ok
                source, target = ends(neg(offset))
                yield inside, pltpu.make_async_remote_copy(
                    src_ref=source,
                    dst_ref=target,
                    send_sem=halo_send.at[e, SLOT[offset]],
                    recv_sem=halo_recv.at[e, SLOT[offset]],
                    device_id=(tx, ty, tz),
                    device_id_type=MESH,
                )

        def begin():
            for inside, copy in copies():
                pl.when(inside)(copy.start)

        def finish():
            for inside, copy in landings():
                pl.when(inside)(copy.wait_recv)
            for inside, copy in copies():
                later.append(functools.partial(pl.when(inside), copy.wait_send))

        return begin, finish

    def tensor_ends(offset):
        dx, dy, dz = offset
        if dz:
            return t_zpack, t_zr.at[ZINDEX[neg(offset)]]
        if dx and dy:
            return t_ypack.at[(dy + 1) // 2, 0], t_xyr.at[XYINDEX[neg(offset)]]
        if dx:
            source, target = (bx, 0) if dx > 0 else (1, bx + 1)
            return tens.at[pl.ds(0, 3), source, pl.ds(TOP, by)], tens.at[
                pl.ds(0, 3), target, pl.ds(TOP, by)
            ]
        return t_ypack.at[(dy + 1) // 2], t_yr.at[(1 - dy) // 2]

    def field_ends(e):
        def ends(offset):
            dx, dy, dz = offset
            if dz:
                return f_zpack.at[e], f_zr.at[e, ZINDEX[neg(offset)]]
            if dx and dy:
                return f_ypack.at[e, (dy + 1) // 2], f_xyr.at[e, XYINDEX[neg(offset)]]
            if dx:
                source, target = (bx, 0) if dx > 0 else (1, bx + 1)
                return field.at[e, source, pl.ds(TOP, by)], field.at[e, target, pl.ds(TOP, by)]
            return f_ypack.at[e, (dy + 1) // 2], f_yr.at[e, (1 - dy) // 2]

        return ends

    spread(msg1, gat1, 0)
    begin, finish = exchange(0, tensor_ends)
    begin()
    finish()

    def corners_in(buffer, arrived):
        for offset in XYOFFSETS:
            dx, dy, _ = offset
            x = bx + 1 if dx > 0 else 0
            y = TOP + by if dy > 0 else TOP - 1
            row = 0 if dx > 0 else hi_x
            buffer[x, y : y + 1, :] = arrived[XYINDEX[offset], row : row + 1, :]

    def lines_in(buffer, arrived, side):
        y = TOP - 1 if side == 0 else TOP + by
        for x in range(bx):
            buffer[1 + x, y : y + 1, :] = arrived[x : x + 1, :]

    def shifted(cells, dz, column):
        turned = pltpu.roll(cells, bz - 1 if dz > 0 else 1, 1)
        edge = bz - 1 if dz > 0 else 0
        return jnp.where(iota(cells.shape, 1) == edge, column, turned)

    def tilt(centre, up, down, arrived, i, lines, with_x, with_y):
        stack = []
        for dz in (1, -1):
            r = i if dz > 0 else i + 3

            def row_of(offset):
                return arrived[ZINDEX[offset], r : r + 1, :]

            stack.append(row_of((0, 0, dz)))
            stack.append(
                jnp.where(lane1 < by, row_of((1, 0, dz)), row_of((-1, 0, dz)))
                if with_x
                else jnp.zeros((1, bz), F32)
            )
            stack.append(
                jnp.where(lane1 % by == 0, row_of((0, 1, dz)), row_of((0, -1, dz)))
                if with_y
                else jnp.zeros((1, bz), F32)
            )
        stack = stack + [jnp.zeros((2, bz), F32)]
        columns = jnp.concatenate(stack, axis=0).T
        cells = centre[own, rows, :].reshape(bx * by, bz)
        for dz, out, k in ((1, up, 0), (-1, down, 3)):
            moved = shifted(cells, dz, columns[:, k : k + 1])
            out[own, rows, :] = moved.reshape(bx, by, bz)
            if with_x:
                out[0, rows, :] = shifted(
                    centre[0, rows, :], dz, columns[hi_x * by : bx * by, k + 1 : k + 2]
                )
                out[bx + 1, rows, :] = shifted(
                    centre[bx + 1, rows, :], dz, columns[0:by, k + 1 : k + 2]
                )
            if with_y:
                for side, at, inner in ((0, TOP - 1, hi_y), (1, TOP + by, 0)):
                    edge = jnp.concatenate(
                        [
                            columns[x * by + inner : x * by + inner + 1, k + 2 : k + 3]
                            for x in range(bx)
                        ],
                        axis=0,
                    )
                    moved = shifted(lines[side], dz, edge)
                    for x in range(bx):
                        out[1 + x, at : at + 1, :] = moved[x : x + 1, :]

    for side in range(2):
        for i, slot in enumerate((XY, YY, YZ)):
            lines_in(tens.at[slot], t_yr.at[side, i], side)
    corners_in(tens.at[XY], t_xyr)
    for slot, with_x, with_y in ((XZ, True, False), (YZ, False, True), (ZZ, False, False)):
        i = ZSLOT[slot]
        tilt(
            tens.at[slot],
            tens_p.at[i],
            tens_m.at[i],
            t_zr,
            i,
            (t_yr[0, 2], t_yr[1, 2]),
            with_x,
            with_y,
        )

    def weigh(t, x):
        dx, dy, dz, slot, factor = TAPS[t]
        here = tens[slot, 1 + x, rows, :]
        there_rows = slice(TOP + dy, TOP + dy + by)
        if dz:
            beside = tens_p if dz > 0 else tens_m
            there = beside[ZSLOT[slot], 1 + x + dx, there_rows, :]
        else:
            there = tens[slot, 1 + x + dx, there_rows, :]
        weight[t, x] = factor * (here + there)

    gathered(gat1, 0)
    for d in range(count):
        den1[d * zblk : (d + 1) * zblk, :] = gat1[d]
    every = den1[...]
    lane_b = iota(every.shape, 1)
    number = every[:, COARSE + 2 : COARSE + 3]
    hot = (lane_b.astype(F32) == number).astype(F32)
    rhs = jnp.sum(every[:, COARSE + 1 : COARSE + 2] * hot, axis=0, keepdims=True)
    parts = jnp.where(lane_b <= COARSE, every, 0.0)
    flow = lax.dot_general(
        hot, parts, (((0,), (0,)), ((), ())), precision=HIGHEST, preferred_element_type=F32
    )
    back = lax.dot_general(
        parts, hot, (((0,), (0,)), ((), ())), precision=HIGHEST, preferred_element_type=F32
    )
    flow, back = flow[0:COARSE], back[0:COARSE]
    row_c, lane_c = iota((COARSE, LANES), 0), iota((COARSE, LANES), 1)
    outward = jnp.sum(flow, axis=1, keepdims=True)
    inward = jnp.sum(flow, axis=0, keepdims=True)
    coarse = jnp.where(row_c == lane_c, outward + inward, 0.0) - flow - back
    work = jnp.where(
        lane_c < COARSE,
        (row_c == lane_c).astype(F32),
        pltpu.roll(jnp.where(lane_c < COARSE, coarse, 0.0), COARSE, 1),
    )
    units = [(t, x) for x in range(bx) for t in range(len(TAPS))]
    share = -(-len(units) * PIVOTS // COARSE)
    for k in range(0, COARSE, PIVOTS):
        columns = [
            jnp.broadcast_to(work[:, COARSE + k + c : COARSE + k + c + 1], (COARSE, LANES))
            for c in range(PIVOTS)
        ]
        lines = [work[k + i : k + i + 1, :] for i in range(PIVOTS)]
        pivot = [[columns[c][k + i : k + i + 1, :] for c in range(PIVOTS)] for i in range(PIVOTS)]
        for unit in units[:share]:
            weigh(*unit)
        units = units[share:]
        for i in range(PIVOTS):
            scale = 1.0 / pivot[i][i]
            lines[i] = lines[i] * scale
            for c in range(i + 1, PIVOTS):
                pivot[i][c] = pivot[i][c] * scale
            for r in range(PIVOTS):
                if r != i:
                    ratio = pivot[r][i]
                    lines[r] = lines[r] - ratio * lines[i]
                    for c in range(i + 1, PIVOTS):
                        pivot[r][c] = pivot[r][c] - ratio * pivot[i][c]
        for c in range(PIVOTS):
            work = work - columns[c] * lines[c]
        for i in range(PIVOTS):
            work = jnp.where(row_c == k + i, lines[i], work)
    for unit in units:
        weigh(*unit)
    inverse[0:COARSE, :] = jnp.where(lane_c < COARSE, work, 0.0)
    inverse[COARSE:LANES, :] = jnp.zeros((LANES - COARSE, LANES), F32)

    reach = [
        jnp.dot(near, inverse[...], precision=HIGHEST, preferred_element_type=F32)
        for near in around
    ]

    def solve(row):
        wide = jnp.broadcast_to(row, (8, LANES))
        got = jnp.dot(wide, inverse[...], precision=HIGHEST, preferred_element_type=F32)
        return got[0:1]

    row16, lane16 = iota((16, LANES), 0), iota((16, LANES), 1)
    place16, block16 = lane16 % span, lane16 // span

    def steps(row):
        flat_rows = jnp.zeros((16, LANES), F32)
        up_rows, down_rows = flat_rows, flat_rows
        for j in range(zblk):
            u = jnp.sum(reach[j] * row, axis=1, keepdims=True)
            mine = block16 == j
            flat_rows = jnp.where(mine, u[16:32], flat_rows)
            up_rows = jnp.where(mine, jnp.where(place16 == span - 1, u[32:48], u[16:32]), up_rows)
            down_rows = jnp.where(mine, jnp.where(place16 == 0, u[0:16], u[16:32]), down_rows)
        centre = flat_rows[4:5]
        return centre, {0: centre - flat_rows, 1: centre - up_rows, -1: centre - down_rows}

    plane_row = iota((by, bz), 0)

    def coarse_image(diffs, x):
        total = jnp.zeros((by, bz), F32)
        for t, (dx, dy, dz, _, _) in enumerate(TAPS):
            ax = 1 if x + dx >= bx else (-1 if x + dx < 0 else 0)

            def line(ay):
                r = (ax + 1) * 3 + ay + 1
                return diffs[dz][r : r + 1]

            if dz == 0 and ax == 0 and dy == 0:
                continue
            if dy == 0:
                delta = jnp.broadcast_to(line(0), (by, bz))
            else:
                delta = jnp.where(
                    plane_row == (hi_y if dy > 0 else 0), line(dy), line(0)
                )
            total = total + weight[t, x] * delta
        return total

    index_f = iota((bx * by, LANES), 0)
    same_f = index_f == iota((bx * by, LANES), 1)

    def begin_field(e):
        cells = field[e, own, rows, :].reshape(bx * by, bz)
        for r, at in ((0, 0), (3, bz - 1)):
            column = jnp.where(same_f, cells[:, at : at + 1], 0.0)
            f_zpack[e, r : r + 1, :] = jnp.sum(column, axis=0, keepdims=True)
        for side, y in ((0, 0), (1, hi_y)):
            for x in range(bx):
                f_ypack[e, side, x : x + 1, :] = field[e, 1 + x, TOP + y : TOP + y + 1, :]
        begin, finish = exchange(1 + e, field_ends(e))
        begin()
        return finish

    def operate(e):
        base = field.at[e]
        for side in range(2):
            lines_in(base, f_yr.at[e, side], side)
        corners_in(base, f_xyr.at[e])
        tilt(
            base, field_p, field_m, f_zr.at[e], 0, (f_yr[e, 0], f_yr[e, 1]), True, True
        )
        norm = jnp.zeros((by, bz), F32)
        cross, total = norm, norm
        for x in range(bx):
            here = base[1 + x, rows, :]
            acc = jnp.zeros((by, bz), F32)
            for t, (dx, dy, dz, _, _) in enumerate(TAPS):
                source = base if dz == 0 else (field_p if dz > 0 else field_m)
                there = source[1 + x + dx, TOP + dy : TOP + dy + by, :]
                acc = acc + weight[t, x] * (here - there)
            prod[x] = acc
            norm = norm + here * here
            cross = cross + here * acc
            total = total + acc
        total = jnp.sum(total, axis=0, keepdims=True)
        lists = [jnp.where(block == j, total, 0.0) for j in range(zblk)]
        lists += [jnp.sum(norm, axis=0, keepdims=True), jnp.sum(cross, axis=0, keepdims=True)]
        sums = jnp.sum(jnp.concatenate(lists, axis=0), axis=1, keepdims=True)
        row = jnp.zeros((1, LANES), F32)
        for i, at in enumerate(own_id + [COARSE, COARSE + 1]):
            row = row + jnp.where(lane1 == at, sums[i : i + 1], 0.0)
        msg2[e] = row
        gat2[e, me] = row
        spread(msg2.at[e], gat2.at[e], 1 + e)

    def collect(e):
        gathered(gat2.at[e], 1 + e)
        terms = [gat2[e, d] for d in range(count)]
        while len(terms) > 1:
            pairs = [a + b for a, b in zip(terms[0::2], terms[1::2])]
            terms = pairs + terms[len(pairs) * 2 :]
        row = terms[0]
        values = solve(row)
        shared = jnp.sum(row * values, axis=1, keepdims=True)
        norm = row[:, COARSE : COARSE + 1]
        cross = row[:, COARSE + 1 : COARSE + 2] - shared
        return row, norm, cross

    centre0, diffs = steps(rhs)
    for x in range(bx):
        field[0, 1 + x, rows, :] = right_ref[x] - coarse_image(diffs, x)
    finish = begin_field(0)
    finish()
    operate(0)
    row0, norm0, curve0 = collect(0)
    centre1, diffs = steps(row0)
    alpha0 = norm0 / curve0
    for x in range(bx):
        moved = prod[x] - coarse_image(diffs, x)
        image[x] = moved
        field[1, 1 + x, rows, :] = field[0, 1 + x, rows, :] - alpha0 * moved
    finish = begin_field(1)
    finish()
    operate(1)
    row1, norm1, curve1 = collect(1)
    centre2, diffs = steps(row1)
    beta = norm1 / norm0
    alpha1 = norm1 / (curve1 - beta * norm1 / alpha0)
    both = alpha0 + alpha1 * beta
    coarse_row = centre0 - both * centre1 - alpha1 * centre2
    for x in range(bx):
        moved = prod[x] - coarse_image(diffs, x) + beta * image[x]
        now = field[1, 1 + x, rows, :]
        res_ref[x] = now - alpha1 * moved
        sol_ref[x] = coarse_row + both * field[0, 1 + x, rows, :] + alpha1 * now
    for wait in later:
        wait()


def solution(mesh):
    nx, ny, nz = (mesh.shape[name] for name in ("gx", "gy", "gz"))
    count = nx * ny * nz

    def body(right_side, fiber_class, conductivity_scale, class_tensor, block_ids):
        bx, by, bz = right_side.shape
        nbx, nby, nbz = block_ids.shape
        zblk = nbz // nz
        dims = (nx, ny, nz, bx, by, zblk, nbx, nby, nbz)
        px, py = bx + 2, by + 16
        vmem = lambda *shape: pltpu.VMEM(shape, F32)
        whole = pl.BlockSpec(memory_space=pltpu.VMEM)
        scalar = pl.BlockSpec(memory_space=pltpu.SMEM)
        return pl.pallas_call(
            functools.partial(kernel, dims),
            out_shape=[jax.ShapeDtypeStruct((bx, by, bz), F32)] * 2,
            in_specs=[scalar, scalar, whole, whole, whole],
            out_specs=[whole, whole],
            scratch_shapes=[
                vmem(6, px, py, bz),
                vmem(3, px, py, bz),
                vmem(3, px, py, bz),
                vmem(18, bx, by, bz),
                vmem(2, px, py, bz),
                vmem(px, py, bz),
                vmem(px, py, bz),
                vmem(bx, by, bz),
                vmem(bx, by, bz),
                vmem(48, bz),
                vmem(LANES, LANES),
                vmem(2, 3, bx, bz),
                vmem(2, 3, bx, bz),
                vmem(4, bx, bz),
                vmem(8, bz),
                vmem(len(ZOFFSETS), 8, bz),
                vmem(2, 2, bx, bz),
                vmem(2, 2, bx, bz),
                vmem(2, 4, bx, bz),
                vmem(2, 8, bz),
                vmem(2, len(ZOFFSETS), 8, bz),
                vmem(zblk, LANES),
                vmem(count, zblk, LANES),
                vmem(count * zblk, LANES),
                vmem(2, 1, LANES),
                vmem(2, count, 1, LANES),
                pltpu.SemaphoreType.DMA((3, 18)),
                pltpu.SemaphoreType.DMA((3, 18)),
                pltpu.SemaphoreType.DMA((3,)),
                pltpu.SemaphoreType.DMA((3,)),
            ],
            compiler_params=pltpu.CompilerParams(collective_id=0, has_side_effects=True),
        )(block_ids, class_tensor, right_side, fiber_class, conductivity_scale)

    placed = (P("gx", "gy", "gz"), P("gx", "gy", "gz"), P("gx", "gy", "gz"), P(), P())
    return jax.shard_map(
        body,
        mesh=mesh,
        in_specs=placed,
        out_specs=(P("gx", "gy", "gz"), P("gx", "gy", "gz")),
        check_vma=False,
    )
```

```python
import functools

import jax
import jax.numpy as jnp
from jax import lax
from jax.experimental import pallas as pl
from jax.experimental.pallas import tpu as pltpu
from jax.sharding import PartitionSpec as P

COARSE = 64
PIVOTS = 4
LANES = 128
HIGHEST = lax.Precision.HIGHEST
MESH = pl.DeviceIdType.MESH
F32 = jnp.float32

XX, XZ, XY, YY, YZ, ZZ = range(6)
TABLE_ROW = {XX: 0, YY: 1, ZZ: 2, XY: 3, XZ: 4, YZ: 5}
ZSLOT = {XZ: 0, YZ: 1, ZZ: 2}

TAPS = (
    (1, 0, 0, XX, 0.5),
    (-1, 0, 0, XX, 0.5),
    (0, 1, 0, YY, 0.5),
    (0, -1, 0, YY, 0.5),
    (0, 0, 1, ZZ, 0.5),
    (0, 0, -1, ZZ, 0.5),
    (1, 1, 0, XY, 0.25),
    (-1, -1, 0, XY, 0.25),
    (1, -1, 0, XY, -0.25),
    (-1, 1, 0, XY, -0.25),
    (1, 0, 1, XZ, 0.25),
    (-1, 0, -1, XZ, 0.25),
    (1, 0, -1, XZ, -0.25),
    (-1, 0, 1, XZ, -0.25),
    (0, 1, 1, YZ, 0.25),
    (0, -1, -1, YZ, 0.25),
    (0, 1, -1, YZ, -0.25),
    (0, -1, 1, YZ, -0.25),
)
OFFSETS = tuple(tap[:3] for tap in TAPS)
FAR_FIRST = OFFSETS[6:] + OFFSETS[:6]
SLOT = {offset: i for i, offset in enumerate(OFFSETS)}
ZOFFSETS = tuple(o for o in OFFSETS if o[2])
ZINDEX = {offset: i for i, offset in enumerate(ZOFFSETS)}
XYOFFSETS = tuple(o for o in OFFSETS if o[0] and o[1])
XYINDEX = {offset: i for i, offset in enumerate(XYOFFSETS)}
TOP = 8


def neg(offset):
    return tuple(-s for s in offset)


def iota(shape, dim):
    return lax.broadcasted_iota(jnp.int32, shape, dim)


def kernel(
    dims,
    ids_ref,
    table_ref,
    right_ref,
    class_ref,
    scale_ref,
    sol_ref,
    res_ref,
    tens,
    tens_p,
    tens_m,
    weight,
    field,
    field_p,
    field_m,
    prod,
    image,
    rim,
    inverse,
    t_ypack,
    t_yr,
    t_xyr,
    t_zpack,
    t_zr,
    f_ypack,
    f_yr,
    f_xyr,
    f_zpack,
    f_zr,
    msg1,
    gat1,
    den1,
    msg2,
    gat2,
    halo_send,
    halo_recv,
    gat_send,
    gat_recv,
):
    nx, ny, nz, bx, by, zblk, nbx, nby, nbz = dims
    bz = LANES
    span = bz // zblk
    count = nx * ny * nz
    px, py, pz = lax.axis_index("gx"), lax.axis_index("gy"), lax.axis_index("gz")
    me = (px * ny + py) * nz + pz
    rows = slice(TOP, TOP + by)
    own = slice(1, 1 + bx)

    tens[0:3, 0, rows, :] = jnp.zeros((3, by, bz), F32)
    tens[0:3, bx + 1, rows, :] = jnp.zeros((3, by, bz), F32)
    for e in range(2):
        field[e, 0, rows, :] = jnp.zeros((by, bz), F32)
        field[e, bx + 1, rows, :] = jnp.zeros((by, bz), F32)
    for buffer in (t_yr, t_xyr, t_zr, f_yr, f_xyr, f_zr):
        buffer[...] = jnp.zeros(buffer.shape, F32)

    def other(d):
        t = lax.rem(me + d, count)
        return (lax.div(t, ny * nz), lax.rem(lax.div(t, nz), ny), lax.rem(t, nz))

    steps_far = sorted(
        (
            (dx, dy, dz)
            for dx in range(nx)
            for dy in range(ny)
            for dz in range(nz)
            if dx or dy or dz
        ),
        key=lambda o: -sum(min(d, n - d) for d, n in zip(o, (nx, ny, nz // 2))),
    )

    def each_peer(action):
        if count > 64:
            pl.loop(1, count)(lambda d: action(other(d)))
            return

        def turned(at, n):
            return [at] + [
                jnp.where(at + d >= n, at + d - n, at + d) for d in range(1, n)
            ]

        xs, ys, zs = turned(px, nx), turned(py, ny), turned(pz, nz)
        for dx, dy, dz in steps_far:
            action((xs[dx], ys[dy], zs[dz]))

    barrier = pltpu.get_barrier_semaphore()

    def greet(peer):
        pl.semaphore_signal(barrier, inc=1, device_id=peer, device_id_type=MESH)

    each_peer(greet)

    lane1 = iota((1, bz), 1)
    place = lane1 % span
    block = lane1 // span
    first, last = place == 0, place == span - 1

    def read_id(x, y, z):
        inside = (x >= 0) & (x < nbx) & (y >= 0) & (y < nby) & (z >= 0) & (z < nbz)
        value = ids_ref[
            jnp.clip(x, 0, nbx - 1), jnp.clip(y, 0, nby - 1), jnp.clip(z, 0, nbz - 1)
        ]
        return jnp.where(inside, value, COARSE)

    window = {}
    for dx in range(3):
        for dy in range(3):
            for dz in range(zblk + 2):
                window[dx, dy, dz] = read_id(px + dx - 1, py + dy - 1, pz * zblk + dz - 1)
    around = []
    row48 = iota((48, LANES), 0)
    lane48 = iota((48, LANES), 1)
    for j in range(zblk):
        ids = jnp.full((48, LANES), -1, jnp.int32)
        for dz in range(3):
            for dx in range(3):
                for dy in range(3):
                    ids = jnp.where(
                        row48 == dz * 16 + dx * 3 + dy, window[dx, dy, j + dz], ids
                    )
        around.append((ids == lane48).astype(F32))
    own_id = [window[1, 1, j + 1] for j in range(zblk)]

    for x in range(bx):
        kind = class_ref[x]
        parts = [jnp.full((by, bz), table_ref[c, 0], F32) for c in range(6)]
        for k in range(1, table_ref.shape[1]):
            match = kind == k
            parts = [jnp.where(match, table_ref[c, k], parts[c]) for c in range(6)]
        for slot in range(6):
            tens[slot, 1 + x, rows, :] = parts[TABLE_ROW[slot]] * scale_ref[x]

    def own_tensor(slot):
        return tens[slot, own, rows, :]

    def halves(row):
        return [
            jnp.sum(jnp.where(block == j, row, 0.0), axis=1, keepdims=True) for j in range(zblk)
        ]

    def plane_sum(slot, x):
        return jnp.sum(tens[slot, 1 + x, rows, :], axis=0, keepdims=True)

    def line_sum(slot, y):
        total = tens[slot, 1, TOP + y : TOP + y + 1, :]
        for x in range(1, bx):
            total = total + tens[slot, 1 + x, TOP + y : TOP + y + 1, :]
        return total

    def corner(x, y):
        return tens[XY, 1 + x, TOP + y : TOP + y + 1, :]

    hi_x, hi_y = bx - 1, by - 1
    c00, c01, c10, c11 = corner(0, 0), corner(0, hi_y), corner(hi_x, 0), corner(hi_x, hi_y)
    xz_lo, xz_hi = plane_sum(XZ, 0), plane_sum(XZ, hi_x)
    yz_lo, yz_hi = line_sum(YZ, 0), line_sum(YZ, hi_y)
    zz_all = jnp.sum(jnp.sum(own_tensor(ZZ), axis=0), axis=0, keepdims=True)
    flat = {
        (1, 0): 0.5 * plane_sum(XX, hi_x) + 0.25 * (c10 - c11),
        (-1, 0): 0.5 * plane_sum(XX, 0) + 0.25 * (c01 - c00),
        (0, 1): 0.5 * line_sum(YY, hi_y) + 0.25 * (c01 - c11),
        (0, -1): 0.5 * line_sum(YY, 0) + 0.25 * (c10 - c00),
        (1, 1): 0.25 * c11,
        (-1, -1): 0.25 * c00,
        (1, -1): -0.25 * c10,
        (-1, 1): -0.25 * c01,
    }
    tilted = {
        (1, 0): 0.25 * xz_hi,
        (-1, 0): -0.25 * xz_lo,
        (0, 1): 0.25 * yz_hi,
        (0, -1): -0.25 * yz_lo,
    }
    slant = 0.25 * (xz_lo - xz_hi + yz_lo - yz_hi)
    rim[...] = jnp.zeros(rim.shape, F32)
    for key, row in flat.items():
        at = (key[0] + 1) * 3 + key[1] + 1
        if key in tilted:
            up = jnp.where(last, tilted[key], 0.0)
            down = jnp.where(first, -tilted[key], 0.0)
            rim[at : at + 1, :] = down
            rim[32 + at : 33 + at, :] = up
            row = row - up - down
        rim[16 + at : 17 + at, :] = row
    rim[4:5, :] = jnp.where(first, 0.5 * zz_all - slant, 0.0)
    rim[36:37, :] = jnp.where(last, 0.5 * zz_all + slant, 0.0)

    sums = jnp.sum(jnp.sum(right_ref[...], axis=0), axis=0, keepdims=True)
    totals = halves(sums)
    block48 = lane48 // span
    for j in range(zblk):
        leaving = jnp.sum(jnp.where(block48 == j, rim[...], 0.0), axis=1, keepdims=True)
        row = jnp.sum(leaving * around[j], axis=0, keepdims=True)
        row = jnp.where(lane1 == COARSE + 1, totals[j], row)
        row = jnp.where(lane1 == COARSE + 2, own_id[j].astype(F32), row)
        msg1[j : j + 1, :] = row
        gat1[me, j : j + 1, :] = row

    lane8, row8 = iota((8, LANES), 1), iota((8, LANES), 0)

    def pick(i):
        return (
            ((row8 == i) & (lane8 == 0)) | ((row8 == i + 3) & (lane8 == bz - 1))
        ).astype(F32)

    def faces(cells, i):
        return lax.dot_general(
            pick(i),
            cells.reshape(bx * by, bz),
            (((1,), (1,)), ((), ())),
            precision=HIGHEST,
            preferred_element_type=F32,
        )

    t_zpack[...] = (
        faces(own_tensor(XZ), 0) + faces(own_tensor(YZ), 1) + faces(own_tensor(ZZ), 2)
    )
    for side, y in ((0, 0), (1, hi_y)):
        for i, slot in enumerate((XY, YY, YZ)):
            for x in range(bx):
                t_ypack[side, i, x : x + 1, :] = tens[slot, 1 + x, TOP + y : TOP + y + 1, :]

    pl.semaphore_wait(barrier, count - 1)

    later = []

    def spread(msg, gat, g):
        def send(peer):
            pltpu.make_async_remote_copy(
                src_ref=msg,
                dst_ref=gat.at[me],
                send_sem=gat_send.at[g],
                recv_sem=gat_recv.at[g],
                device_id=peer,
                device_id_type=MESH,
            ).start()

        each_peer(send)

    def gathered(gat, g):
        every = pltpu.make_async_remote_copy(
            src_ref=gat.at[pl.ds(0, count - 1)],
            dst_ref=gat.at[pl.ds(0, count - 1)],
            send_sem=gat_send.at[g],
            recv_sem=gat_recv.at[g],
            device_id=other(1),
            device_id_type=MESH,
        )
        every.wait_recv()
        later.append(every.wait_send)

    def exchange(e, ends):
        def copies():
            for offset in FAR_FIRST:
                dx, dy, dz = offset
                tx, ty, tz = px + dx, py + dy, pz + dz
                inside = None
                for step, at, size in ((dx, tx, nx), (dy, ty, ny), (dz, tz, nz)):
                    if step:
                        ok = (at < size) if step > 0 else (at >= 0)
                        inside = ok if inside is None else inside & ok
                source, target = ends(offset)
                yield inside, pltpu.make_async_remote_copy(
                    src_ref=source,
                    dst_ref=target,
                    send_sem=halo_send.at[e, SLOT[offset]],
                    recv_sem=halo_recv.at[e, SLOT[neg(offset)]],
                    device_id=(tx, ty, tz),
                    device_id_type=MESH,
                )

        def landings():
            for offset in FAR_FIRST:
                dx, dy, dz = offset
                tx, ty, tz = px + dx, py + dy, pz + dz
                inside = None
                for step, at, size in ((dx, tx, nx), (dy, ty, ny), (dz, tz, nz)):
                    if step:
                        ok = (at < size) if step > 0 else (at >= 0)
                        inside = ok if inside is None else inside & ok
                source, target = ends(neg(offset))
                yield inside, pltpu.make_async_remote_copy(
                    src_ref=source,
                    dst_ref=target,
                    send_sem=halo_send.at[e, SLOT[offset]],
                    recv_sem=halo_recv.at[e, SLOT[offset]],
                    device_id=(tx, ty, tz),
                    device_id_type=MESH,
                )

        def begin():
            for inside, copy in copies():
                pl.when(inside)(copy.start)

        def finish():
            for inside, copy in landings():
                pl.when(inside)(copy.wait_recv)
            for inside, copy in copies():
                later.append(functools.partial(pl.when(inside), copy.wait_send))

        return begin, finish

    def tensor_ends(offset):
        dx, dy, dz = offset
        if dz:
            return t_zpack, t_zr.at[ZINDEX[neg(offset)]]
        if dx and dy:
            return t_ypack.at[(dy + 1) // 2, 0], t_xyr.at[XYINDEX[neg(offset)]]
        if dx:
            source, target = (bx, 0) if dx > 0 else (1, bx + 1)
            return tens.at[pl.ds(0, 3), source, pl.ds(TOP, by)], tens.at[
                pl.ds(0, 3), target, pl.ds(TOP, by)
            ]
        return t_ypack.at[(dy + 1) // 2], t_yr.at[(1 - dy) // 2]

    def field_ends(e):
        def ends(offset):
            dx, dy, dz = offset
            if dz:
                return f_zpack.at[e], f_zr.at[e, ZINDEX[neg(offset)]]
            if dx and dy:
                return f_ypack.at[e, (dy + 1) // 2], f_xyr.at[e, XYINDEX[neg(offset)]]
            if dx:
                source, target = (bx, 0) if dx > 0 else (1, bx + 1)
                return field.at[e, source, pl.ds(TOP, by)], field.at[e, target, pl.ds(TOP, by)]
            return f_ypack.at[e, (dy + 1) // 2], f_yr.at[e, (1 - dy) // 2]

        return ends

    spread(msg1, gat1, 0)
    begin, finish = exchange(0, tensor_ends)
    begin()
    finish()

    def corners_in(buffer, arrived):
        for offset in XYOFFSETS:
            dx, dy, _ = offset
            x = bx + 1 if dx > 0 else 0
            y = TOP + by if dy > 0 else TOP - 1
            row = 0 if dx > 0 else hi_x
            buffer[x, y : y + 1, :] = arrived[XYINDEX[offset], row : row + 1, :]

    def lines_in(buffer, arrived, side):
        y = TOP - 1 if side == 0 else TOP + by
        for x in range(bx):
            buffer[1 + x, y : y + 1, :] = arrived[x : x + 1, :]

    def shifted(cells, dz, column):
        turned = pltpu.roll(cells, bz - 1 if dz > 0 else 1, 1)
        edge = bz - 1 if dz > 0 else 0
        return jnp.where(iota(cells.shape, 1) == edge, column, turned)

    def tilt(centre, up, down, arrived, i, lines, with_x, with_y):
        stack = []
        for dz in (1, -1):
            r = i if dz > 0 else i + 3

            def row_of(offset):
                return arrived[ZINDEX[offset], r : r + 1, :]

            stack.append(row_of((0, 0, dz)))
            stack.append(
                jnp.where(lane1 < by, row_of((1, 0, dz)), row_of((-1, 0, dz)))
                if with_x
                else jnp.zeros((1, bz), F32)
            )
            stack.append(
                jnp.where(lane1 % by == 0, row_of((0, 1, dz)), row_of((0, -1, dz)))
                if with_y
                else jnp.zeros((1, bz), F32)
            )
        stack = stack + [jnp.zeros((2, bz), F32)]
        columns = jnp.concatenate(stack, axis=0).T
        cells = centre[own, rows, :].reshape(bx * by, bz)
        for dz, out, k in ((1, up, 0), (-1, down, 3)):
            moved = shifted(cells, dz, columns[:, k : k + 1])
            out[own, rows, :] = moved.reshape(bx, by, bz)
            if with_x:
                out[0, rows, :] = shifted(
                    centre[0, rows, :], dz, columns[hi_x * by : bx * by, k + 1 : k + 2]
                )
                out[bx + 1, rows, :] = shifted(
                    centre[bx + 1, rows, :], dz, columns[0:by, k + 1 : k + 2]
                )
            if with_y:
                for side, at, inner in ((0, TOP - 1, hi_y), (1, TOP + by, 0)):
                    edge = jnp.concatenate(
                        [
                            columns[x * by + inner : x * by + inner + 1, k + 2 : k + 3]
                            for x in range(bx)
                        ],
                        axis=0,
                    )
                    moved = shifted(lines[side], dz, edge)
                    for x in range(bx):
                        out[1 + x, at : at + 1, :] = moved[x : x + 1, :]

    for side in range(2):
        for i, slot in enumerate((XY, YY, YZ)):
            lines_in(tens.at[slot], t_yr.at[side, i], side)
    corners_in(tens.at[XY], t_xyr)
    for slot, with_x, with_y in ((XZ, True, False), (YZ, False, True), (ZZ, False, False)):
        i = ZSLOT[slot]
        tilt(
            tens.at[slot],
            tens_p.at[i],
            tens_m.at[i],
            t_zr,
            i,
            (t_yr[0, 2], t_yr[1, 2]),
            with_x,
            with_y,
        )

    def weigh(t, x):
        dx, dy, dz, slot, factor = TAPS[t]
        here = tens[slot, 1 + x, rows, :]
        there_rows = slice(TOP + dy, TOP + dy + by)
        if dz:
            beside = tens_p if dz > 0 else tens_m
            there = beside[ZSLOT[slot], 1 + x + dx, there_rows, :]
        else:
            there = tens[slot, 1 + x + dx, there_rows, :]
        weight[t, x] = factor * (here + there)

    gathered(gat1, 0)
    for d in range(count):
        den1[d * zblk : (d + 1) * zblk, :] = gat1[d]
    every = den1[...]
    lane_b = iota(every.shape, 1)
    number = every[:, COARSE + 2 : COARSE + 3]
    hot = (lane_b.astype(F32) == number).astype(F32)
    rhs = jnp.sum(every[:, COARSE + 1 : COARSE + 2] * hot, axis=0, keepdims=True)
    parts = jnp.where(lane_b <= COARSE, every, 0.0)
    flow = lax.dot_general(
        hot, parts, (((0,), (0,)), ((), ())), precision=HIGHEST, preferred_element_type=F32
    )
    back = lax.dot_general(
        parts, hot, (((0,), (0,)), ((), ())), precision=HIGHEST, preferred_element_type=F32
    )
    flow, back = flow[0:COARSE], back[0:COARSE]
    row_c, lane_c = iota((COARSE, LANES), 0), iota((COARSE, LANES), 1)
    outward = jnp.sum(flow, axis=1, keepdims=True)
    inward = jnp.sum(flow, axis=0, keepdims=True)
    coarse = jnp.where(row_c == lane_c, outward + inward, 0.0) - flow - back
    work = jnp.where(
        lane_c < COARSE,
        (row_c == lane_c).astype(F32),
        pltpu.roll(jnp.where(lane_c < COARSE, coarse, 0.0), COARSE, 1),
    )
    units = [(t, x) for x in range(bx) for t in range(len(TAPS))]
    share = -(-len(units) * PIVOTS // COARSE)
    for k in range(0, COARSE, PIVOTS):
        columns = [
            jnp.broadcast_to(work[:, COARSE + k + c : COARSE + k + c + 1], (COARSE, LANES))
            for c in range(PIVOTS)
        ]
        lines = [work[k + i : k + i + 1, :] for i in range(PIVOTS)]
        pivot = [[columns[c][k + i : k + i + 1, :] for c in range(PIVOTS)] for i in range(PIVOTS)]
        for unit in units[:share]:
            weigh(*unit)
        units = units[share:]
        for i in range(PIVOTS):
            scale = 1.0 / pivot[i][i]
            lines[i] = lines[i] * scale
            for c in range(i + 1, PIVOTS):
                pivot[i][c] = pivot[i][c] * scale
            for r in range(PIVOTS):
                if r != i:
                    ratio = pivot[r][i]
                    lines[r] = lines[r] - ratio * lines[i]
                    for c in range(i + 1, PIVOTS):
                        pivot[r][c] = pivot[r][c] - ratio * pivot[i][c]
        for c in range(PIVOTS):
            work = work - columns[c] * lines[c]
        for i in range(PIVOTS):
            work = jnp.where(row_c == k + i, lines[i], work)
    for unit in units:
        weigh(*unit)
    inverse[0:COARSE, :] = jnp.where(lane_c < COARSE, work, 0.0)
    inverse[COARSE:LANES, :] = jnp.zeros((LANES - COARSE, LANES), F32)

    reach = [
        jnp.dot(near, inverse[...], precision=HIGHEST, preferred_element_type=F32)
        for near in around
    ]

    def solve(row):
        wide = jnp.broadcast_to(row, (8, LANES))
        got = jnp.dot(wide, inverse[...], precision=HIGHEST, preferred_element_type=F32)
        return got[0:1]

    row16, lane16 = iota((16, LANES), 0), iota((16, LANES), 1)
    place16, block16 = lane16 % span, lane16 // span

    def steps(row):
        flat_rows = jnp.zeros((16, LANES), F32)
        up_rows, down_rows = flat_rows, flat_rows
        for j in range(zblk):
            u = jnp.sum(reach[j] * row, axis=1, keepdims=True)
            mine = block16 == j
            flat_rows = jnp.where(mine, u[16:32], flat_rows)
            up_rows = jnp.where(mine, jnp.where(place16 == span - 1, u[32:48], u[16:32]), up_rows)
            down_rows = jnp.where(mine, jnp.where(place16 == 0, u[0:16], u[16:32]), down_rows)
        centre = flat_rows[4:5]
        return centre, {0: centre - flat_rows, 1: centre - up_rows, -1: centre - down_rows}

    plane_row = iota((by, bz), 0)

    def coarse_image(diffs, x):
        total = jnp.zeros((by, bz), F32)
        for t, (dx, dy, dz, _, _) in enumerate(TAPS):
            ax = 1 if x + dx >= bx else (-1 if x + dx < 0 else 0)

            def line(ay):
                r = (ax + 1) * 3 + ay + 1
                return diffs[dz][r : r + 1]

            if dz == 0 and ax == 0 and dy == 0:
                continue
            if dy == 0:
                delta = jnp.broadcast_to(line(0), (by, bz))
            else:
                delta = jnp.where(
                    plane_row == (hi_y if dy > 0 else 0), line(dy), line(0)
                )
            total = total + weight[t, x] * delta
        return total

    index_f = iota((bx * by, LANES), 0)
    same_f = index_f == iota((bx * by, LANES), 1)

    def begin_field(e):
        cells = field[e, own, rows, :].reshape(bx * by, bz)
        for r, at in ((0, 0), (3, bz - 1)):
            column = jnp.where(same_f, cells[:, at : at + 1], 0.0)
            f_zpack[e, r : r + 1, :] = jnp.sum(column, axis=0, keepdims=True)
        for side, y in ((0, 0), (1, hi_y)):
            for x in range(bx):
                f_ypack[e, side, x : x + 1, :] = field[e, 1 + x, TOP + y : TOP + y + 1, :]
        begin, finish = exchange(1 + e, field_ends(e))
        begin()
        return finish

    def operate(e):
        base = field.at[e]
        for side in range(2):
            lines_in(base, f_yr.at[e, side], side)
        corners_in(base, f_xyr.at[e])
        tilt(
            base, field_p, field_m, f_zr.at[e], 0, (f_yr[e, 0], f_yr[e, 1]), True, True
        )
        norm = jnp.zeros((by, bz), F32)
        cross, total = norm, norm
        for x in range(bx):
            here = base[1 + x, rows, :]
            acc = jnp.zeros((by, bz), F32)
            for t, (dx, dy, dz, _, _) in enumerate(TAPS):
                source = base if dz == 0 else (field_p if dz > 0 else field_m)
                there = source[1 + x + dx, TOP + dy : TOP + dy + by, :]
                acc = acc + weight[t, x] * (here - there)
            prod[x] = acc
            norm = norm + here * here
            cross = cross + here * acc
            total = total + acc
        total = jnp.sum(total, axis=0, keepdims=True)
        lists = [jnp.where(block == j, total, 0.0) for j in range(zblk)]
        lists += [jnp.sum(norm, axis=0, keepdims=True), jnp.sum(cross, axis=0, keepdims=True)]
        sums = jnp.sum(jnp.concatenate(lists, axis=0), axis=1, keepdims=True)
        row = jnp.zeros((1, LANES), F32)
        for i, at in enumerate(own_id + [COARSE, COARSE + 1]):
            row = row + jnp.where(lane1 == at, sums[i : i + 1], 0.0)
        msg2[e] = row
        gat2[e, me] = row
        spread(msg2.at[e], gat2.at[e], 1 + e)

    def collect(e):
        gathered(gat2.at[e], 1 + e)
        terms = [gat2[e, d] for d in range(count)]
        while len(terms) > 1:
            pairs = [a + b for a, b in zip(terms[0::2], terms[1::2])]
            terms = pairs + terms[len(pairs) * 2 :]
        row = terms[0]
        values = solve(row)
        shared = jnp.sum(row * values, axis=1, keepdims=True)
        norm = row[:, COARSE : COARSE + 1]
        cross = row[:, COARSE + 1 : COARSE + 2] - shared
        return row, norm, cross

    centre0, diffs = steps(rhs)
    for x in range(bx):
        field[0, 1 + x, rows, :] = right_ref[x] - coarse_image(diffs, x)
    finish = begin_field(0)
    finish()
    operate(0)
    row0, norm0, curve0 = collect(0)
    centre1, diffs = steps(row0)
    alpha0 = norm0 / curve0
    for x in range(bx):
        moved = prod[x] - coarse_image(diffs, x)
        image[x] = moved
        field[1, 1 + x, rows, :] = field[0, 1 + x, rows, :] - alpha0 * moved
    finish = begin_field(1)
    finish()
    operate(1)
    row1, norm1, curve1 = collect(1)
    centre2, diffs = steps(row1)
    beta = norm1 / norm0
    alpha1 = norm1 / (curve1 - beta * norm1 / alpha0)
    both = alpha0 + alpha1 * beta
    coarse_row = centre0 - both * centre1 - alpha1 * centre2
    for x in range(bx):
        moved = prod[x] - coarse_image(diffs, x) + beta * image[x]
        now = field[1, 1 + x, rows, :]
        res_ref[x] = now - alpha1 * moved
        sol_ref[x] = coarse_row + both * field[0, 1 + x, rows, :] + alpha1 * now
    for wait in later:
        wait()


def solution(mesh):
    nx, ny, nz = (mesh.shape[name] for name in ("gx", "gy", "gz"))
    count = nx * ny * nz

    def body(right_side, fiber_class, conductivity_scale, class_tensor, block_ids):
        bx, by, bz = right_side.shape
        nbx, nby, nbz = block_ids.shape
        zblk = nbz // nz
        dims = (nx, ny, nz, bx, by, zblk, nbx, nby, nbz)
        px, py = bx + 2, by + 16
        vmem = lambda *shape: pltpu.VMEM(shape, F32)
        whole = pl.BlockSpec(memory_space=pltpu.VMEM)
        scalar = pl.BlockSpec(memory_space=pltpu.SMEM)
        return pl.pallas_call(
            functools.partial(kernel, dims),
            out_shape=[jax.ShapeDtypeStruct((bx, by, bz), F32)] * 2,
            in_specs=[scalar, scalar, whole, whole, whole],
            out_specs=[whole, whole],
            scratch_shapes=[
                vmem(6, px, py, bz),
                vmem(3, px, py, bz),
                vmem(3, px, py, bz),
                vmem(18, bx, by, bz),
                vmem(2, px, py, bz),
                vmem(px, py, bz),
                vmem(px, py, bz),
                vmem(bx, by, bz),
                vmem(bx, by, bz),
                vmem(48, bz),
                vmem(LANES, LANES),
                vmem(2, 3, bx, bz),
                vmem(2, 3, bx, bz),
                vmem(4, bx, bz),
                vmem(8, bz),
                vmem(len(ZOFFSETS), 8, bz),
                vmem(2, 2, bx, bz),
                vmem(2, 2, bx, bz),
                vmem(2, 4, bx, bz),
                vmem(2, 8, bz),
                vmem(2, len(ZOFFSETS), 8, bz),
                vmem(zblk, LANES),
                vmem(count, zblk, LANES),
                vmem(count * zblk, LANES),
                vmem(2, 1, LANES),
                vmem(2, count, 1, LANES),
                pltpu.SemaphoreType.DMA((3, 18)),
                pltpu.SemaphoreType.DMA((3, 18)),
                pltpu.SemaphoreType.DMA((3,)),
                pltpu.SemaphoreType.DMA((3,)),
            ],
            compiler_params=pltpu.CompilerParams(
                collective_id=0, has_side_effects=True, vmem_limit_bytes=16 * 1024 * 1024
            ),
        )(block_ids, class_tensor, right_side, fiber_class, conductivity_scale)

    placed = (P("gx", "gy", "gz"), P("gx", "gy", "gz"), P("gx", "gy", "gz"), P(), P())
    return jax.shard_map(
        body,
        mesh=mesh,
        in_specs=placed,
        out_specs=(P("gx", "gy", "gz"), P("gx", "gy", "gz")),
        check_vma=False,
    )
```

```python
import functools

import jax
import jax.numpy as jnp
from jax import lax
from jax.experimental import pallas as pl
from jax.experimental.pallas import tpu as pltpu
from jax.sharding import PartitionSpec as P

COARSE = 64
PIVOTS = 4
LANES = 128
HIGHEST = lax.Precision.HIGHEST
MESH = pl.DeviceIdType.MESH
F32 = jnp.float32

XX, XZ, XY, YY, YZ, ZZ = range(6)
TABLE_ROW = {XX: 0, YY: 1, ZZ: 2, XY: 3, XZ: 4, YZ: 5}
ZSLOT = {XZ: 0, YZ: 1, ZZ: 2}

TAPS = (
    (1, 0, 0, XX, 0.5),
    (-1, 0, 0, XX, 0.5),
    (0, 1, 0, YY, 0.5),
    (0, -1, 0, YY, 0.5),
    (0, 0, 1, ZZ, 0.5),
    (0, 0, -1, ZZ, 0.5),
    (1, 1, 0, XY, 0.25),
    (-1, -1, 0, XY, 0.25),
    (1, -1, 0, XY, -0.25),
    (-1, 1, 0, XY, -0.25),
    (1, 0, 1, XZ, 0.25),
    (-1, 0, -1, XZ, 0.25),
    (1, 0, -1, XZ, -0.25),
    (-1, 0, 1, XZ, -0.25),
    (0, 1, 1, YZ, 0.25),
    (0, -1, -1, YZ, 0.25),
    (0, 1, -1, YZ, -0.25),
    (0, -1, 1, YZ, -0.25),
)
OFFSETS = tuple(tap[:3] for tap in TAPS)
FAR_FIRST = OFFSETS[6:] + OFFSETS[:6]
SLOT = {offset: i for i, offset in enumerate(OFFSETS)}
ZOFFSETS = tuple(o for o in OFFSETS if o[2])
ZINDEX = {offset: i for i, offset in enumerate(ZOFFSETS)}
XYOFFSETS = tuple(o for o in OFFSETS if o[0] and o[1])
XYINDEX = {offset: i for i, offset in enumerate(XYOFFSETS)}
TOP = 8


def neg(offset):
    return tuple(-s for s in offset)


def iota(shape, dim):
    return lax.broadcasted_iota(jnp.int32, shape, dim)


def kernel(
    dims,
    ids_in,
    table_in,
    right_in,
    class_in,
    scale_in,
    sol_ref,
    res_ref,
    ids_ref,
    table_ref,
    right_ref,
    class_ref,
    scale_ref,
    load_sem,
    tens,
    tens_p,
    tens_m,
    weight,
    field,
    field_p,
    field_m,
    prod,
    image,
    rim,
    inverse,
    t_ypack,
    t_yr,
    t_xyr,
    t_zpack,
    t_zr,
    f_ypack,
    f_yr,
    f_xyr,
    f_zpack,
    f_zr,
    msg1,
    gat1,
    den1,
    msg2,
    gat2,
    halo_send,
    halo_recv,
    gat_send,
    gat_recv,
):
    nx, ny, nz, bx, by, zblk, nbx, nby, nbz = dims
    bz = LANES
    span = bz // zblk
    count = nx * ny * nz
    px, py, pz = lax.axis_index("gx"), lax.axis_index("gy"), lax.axis_index("gz")
    me = (px * ny + py) * nz + pz
    rows = slice(TOP, TOP + by)
    own = slice(1, 1 + bx)

    loads = [
        pltpu.make_async_copy(source, target, load_sem.at[i])
        for i, (source, target) in enumerate(
            (
                (table_in, table_ref),
                (ids_in, ids_ref),
                (class_in, class_ref),
                (scale_in, scale_ref),
                (right_in, right_ref),
            )
        )
    ]
    for load in loads:
        load.start()

    tens[0:3, 0, rows, :] = jnp.zeros((3, by, bz), F32)
    tens[0:3, bx + 1, rows, :] = jnp.zeros((3, by, bz), F32)
    for e in range(2):
        field[e, 0, rows, :] = jnp.zeros((by, bz), F32)
        field[e, bx + 1, rows, :] = jnp.zeros((by, bz), F32)
    for buffer in (t_yr, t_xyr, t_zr, f_yr, f_xyr, f_zr):
        buffer[...] = jnp.zeros(buffer.shape, F32)

    def other(d):
        t = lax.rem(me + d, count)
        return (lax.div(t, ny * nz), lax.rem(lax.div(t, nz), ny), lax.rem(t, nz))

    steps_far = sorted(
        (
            (dx, dy, dz)
            for dx in range(nx)
            for dy in range(ny)
            for dz in range(nz)
            if dx or dy or dz
        ),
        key=lambda o: -sum(min(d, n - d) for d, n in zip(o, (nx, ny, nz // 2))),
    )

    def each_peer(action):
        if count > 64:
            pl.loop(1, count)(lambda d: action(other(d)))
            return

        def turned(at, n):
            return [at] + [
                jnp.where(at + d >= n, at + d - n, at + d) for d in range(1, n)
            ]

        xs, ys, zs = turned(px, nx), turned(py, ny), turned(pz, nz)
        for dx, dy, dz in steps_far:
            action((xs[dx], ys[dy], zs[dz]))

    barrier = pltpu.get_barrier_semaphore()

    def greet(peer):
        pl.semaphore_signal(barrier, inc=1, device_id=peer, device_id_type=MESH)

    each_peer(greet)
    for load in loads:
        load.wait()

    lane1 = iota((1, bz), 1)
    place = lane1 % span
    block = lane1 // span
    first, last = place == 0, place == span - 1

    def read_id(x, y, z):
        inside = (x >= 0) & (x < nbx) & (y >= 0) & (y < nby) & (z >= 0) & (z < nbz)
        value = ids_ref[
            jnp.clip(x, 0, nbx - 1), jnp.clip(y, 0, nby - 1), jnp.clip(z, 0, nbz - 1)
        ]
        return jnp.where(inside, value, COARSE)

    window = {}
    for dx in range(3):
        for dy in range(3):
            for dz in range(zblk + 2):
                window[dx, dy, dz] = read_id(px + dx - 1, py + dy - 1, pz * zblk + dz - 1)
    around = []
    row48 = iota((48, LANES), 0)
    lane48 = iota((48, LANES), 1)
    for j in range(zblk):
        ids = jnp.full((48, LANES), -1, jnp.int32)
        for dz in range(3):
            for dx in range(3):
                for dy in range(3):
                    ids = jnp.where(
                        row48 == dz * 16 + dx * 3 + dy, window[dx, dy, j + dz], ids
                    )
        around.append((ids == lane48).astype(F32))
    own_id = [window[1, 1, j + 1] for j in range(zblk)]

    for x in range(bx):
        kind = class_ref[x]
        parts = [jnp.full((by, bz), table_ref[c, 0], F32) for c in range(6)]
        for k in range(1, table_ref.shape[1]):
            match = kind == k
            parts = [jnp.where(match, table_ref[c, k], parts[c]) for c in range(6)]
        for slot in range(6):
            tens[slot, 1 + x, rows, :] = parts[TABLE_ROW[slot]] * scale_ref[x]

    def own_tensor(slot):
        return tens[slot, own, rows, :]

    def halves(row):
        return [
            jnp.sum(jnp.where(block == j, row, 0.0), axis=1, keepdims=True) for j in range(zblk)
        ]

    def plane_sum(slot, x):
        return jnp.sum(tens[slot, 1 + x, rows, :], axis=0, keepdims=True)

    def line_sum(slot, y):
        total = tens[slot, 1, TOP + y : TOP + y + 1, :]
        for x in range(1, bx):
            total = total + tens[slot, 1 + x, TOP + y : TOP + y + 1, :]
        return total

    def corner(x, y):
        return tens[XY, 1 + x, TOP + y : TOP + y + 1, :]

    hi_x, hi_y = bx - 1, by - 1
    c00, c01, c10, c11 = corner(0, 0), corner(0, hi_y), corner(hi_x, 0), corner(hi_x, hi_y)
    xz_lo, xz_hi = plane_sum(XZ, 0), plane_sum(XZ, hi_x)
    yz_lo, yz_hi = line_sum(YZ, 0), line_sum(YZ, hi_y)
    zz_all = jnp.sum(jnp.sum(own_tensor(ZZ), axis=0), axis=0, keepdims=True)
    flat = {
        (1, 0): 0.5 * plane_sum(XX, hi_x) + 0.25 * (c10 - c11),
        (-1, 0): 0.5 * plane_sum(XX, 0) + 0.25 * (c01 - c00),
        (0, 1): 0.5 * line_sum(YY, hi_y) + 0.25 * (c01 - c11),
        (0, -1): 0.5 * line_sum(YY, 0) + 0.25 * (c10 - c00),
        (1, 1): 0.25 * c11,
        (-1, -1): 0.25 * c00,
        (1, -1): -0.25 * c10,
        (-1, 1): -0.25 * c01,
    }
    tilted = {
        (1, 0): 0.25 * xz_hi,
        (-1, 0): -0.25 * xz_lo,
        (0, 1): 0.25 * yz_hi,
        (0, -1): -0.25 * yz_lo,
    }
    slant = 0.25 * (xz_lo - xz_hi + yz_lo - yz_hi)
    rim[...] = jnp.zeros(rim.shape, F32)
    for key, row in flat.items():
        at = (key[0] + 1) * 3 + key[1] + 1
        if key in tilted:
            up = jnp.where(last, tilted[key], 0.0)
            down = jnp.where(first, -tilted[key], 0.0)
            rim[at : at + 1, :] = down
            rim[32 + at : 33 + at, :] = up
            row = row - up - down
        rim[16 + at : 17 + at, :] = row
    rim[4:5, :] = jnp.where(first, 0.5 * zz_all - slant, 0.0)
    rim[36:37, :] = jnp.where(last, 0.5 * zz_all + slant, 0.0)

    sums = jnp.sum(jnp.sum(right_ref[...], axis=0), axis=0, keepdims=True)
    totals = halves(sums)
    block48 = lane48 // span
    for j in range(zblk):
        leaving = jnp.sum(jnp.where(block48 == j, rim[...], 0.0), axis=1, keepdims=True)
        row = jnp.sum(leaving * around[j], axis=0, keepdims=True)
        row = jnp.where(lane1 == COARSE + 1, totals[j], row)
        row = jnp.where(lane1 == COARSE + 2, own_id[j].astype(F32), row)
        msg1[j : j + 1, :] = row
        gat1[me, j : j + 1, :] = row

    lane8, row8 = iota((8, LANES), 1), iota((8, LANES), 0)

    def pick(i):
        return (
            ((row8 == i) & (lane8 == 0)) | ((row8 == i + 3) & (lane8 == bz - 1))
        ).astype(F32)

    def faces(cells, i):
        return lax.dot_general(
            pick(i),
            cells.reshape(bx * by, bz),
            (((1,), (1,)), ((), ())),
            precision=HIGHEST,
            preferred_element_type=F32,
        )

    t_zpack[...] = (
        faces(own_tensor(XZ), 0) + faces(own_tensor(YZ), 1) + faces(own_tensor(ZZ), 2)
    )
    for side, y in ((0, 0), (1, hi_y)):
        for i, slot in enumerate((XY, YY, YZ)):
            for x in range(bx):
                t_ypack[side, i, x : x + 1, :] = tens[slot, 1 + x, TOP + y : TOP + y + 1, :]

    pl.semaphore_wait(barrier, count - 1)

    later = []

    def spread(msg, gat, g):
        def send(peer):
            pltpu.make_async_remote_copy(
                src_ref=msg,
                dst_ref=gat.at[me],
                send_sem=gat_send.at[g],
                recv_sem=gat_recv.at[g],
                device_id=peer,
                device_id_type=MESH,
            ).start()

        each_peer(send)

    def gathered(gat, g):
        every = pltpu.make_async_remote_copy(
            src_ref=gat.at[pl.ds(0, count - 1)],
            dst_ref=gat.at[pl.ds(0, count - 1)],
            send_sem=gat_send.at[g],
            recv_sem=gat_recv.at[g],
            device_id=other(1),
            device_id_type=MESH,
        )
        every.wait_recv()
        later.append(every.wait_send)

    def exchange(e, ends):
        def copies():
            for offset in FAR_FIRST:
                dx, dy, dz = offset
                tx, ty, tz = px + dx, py + dy, pz + dz
                inside = None
                for step, at, size in ((dx, tx, nx), (dy, ty, ny), (dz, tz, nz)):
                    if step:
                        ok = (at < size) if step > 0 else (at >= 0)
                        inside = ok if inside is None else inside & ok
                source, target = ends(offset)
                yield inside, pltpu.make_async_remote_copy(
                    src_ref=source,
                    dst_ref=target,
                    send_sem=halo_send.at[e, SLOT[offset]],
                    recv_sem=halo_recv.at[e, SLOT[neg(offset)]],
                    device_id=(tx, ty, tz),
                    device_id_type=MESH,
                )

        def landings():
            for offset in FAR_FIRST:
                dx, dy, dz = offset
                tx, ty, tz = px + dx, py + dy, pz + dz
                inside = None
                for step, at, size in ((dx, tx, nx), (dy, ty, ny), (dz, tz, nz)):
                    if step:
                        ok = (at < size) if step > 0 else (at >= 0)
                        inside = ok if inside is None else inside & ok
                source, target = ends(neg(offset))
                yield inside, pltpu.make_async_remote_copy(
                    src_ref=source,
                    dst_ref=target,
                    send_sem=halo_send.at[e, SLOT[offset]],
                    recv_sem=halo_recv.at[e, SLOT[offset]],
                    device_id=(tx, ty, tz),
                    device_id_type=MESH,
                )

        def begin():
            for inside, copy in copies():
                pl.when(inside)(copy.start)

        def finish():
            for inside, copy in landings():
                pl.when(inside)(copy.wait_recv)
            for inside, copy in copies():
                later.append(functools.partial(pl.when(inside), copy.wait_send))

        return begin, finish

    def tensor_ends(offset):
        dx, dy, dz = offset
        if dz:
            return t_zpack, t_zr.at[ZINDEX[neg(offset)]]
        if dx and dy:
            return t_ypack.at[(dy + 1) // 2, 0], t_xyr.at[XYINDEX[neg(offset)]]
        if dx:
            source, target = (bx, 0) if dx > 0 else (1, bx + 1)
            return tens.at[pl.ds(0, 3), source, pl.ds(TOP, by)], tens.at[
                pl.ds(0, 3), target, pl.ds(TOP, by)
            ]
        return t_ypack.at[(dy + 1) // 2], t_yr.at[(1 - dy) // 2]

    def field_ends(e):
        def ends(offset):
            dx, dy, dz = offset
            if dz:
                return f_zpack.at[e], f_zr.at[e, ZINDEX[neg(offset)]]
            if dx and dy:
                return f_ypack.at[e, (dy + 1) // 2], f_xyr.at[e, XYINDEX[neg(offset)]]
            if dx:
                source, target = (bx, 0) if dx > 0 else (1, bx + 1)
                return field.at[e, source, pl.ds(TOP, by)], field.at[e, target, pl.ds(TOP, by)]
            return f_ypack.at[e, (dy + 1) // 2], f_yr.at[e, (1 - dy) // 2]

        return ends

    spread(msg1, gat1, 0)
    begin, finish = exchange(0, tensor_ends)
    begin()
    finish()

    def corners_in(buffer, arrived):
        for offset in XYOFFSETS:
            dx, dy, _ = offset
            x = bx + 1 if dx > 0 else 0
            y = TOP + by if dy > 0 else TOP - 1
            row = 0 if dx > 0 else hi_x
            buffer[x, y : y + 1, :] = arrived[XYINDEX[offset], row : row + 1, :]

    def lines_in(buffer, arrived, side):
        y = TOP - 1 if side == 0 else TOP + by
        for x in range(bx):
            buffer[1 + x, y : y + 1, :] = arrived[x : x + 1, :]

    def shifted(cells, dz, column):
        turned = pltpu.roll(cells, bz - 1 if dz > 0 else 1, 1)
        edge = bz - 1 if dz > 0 else 0
        return jnp.where(iota(cells.shape, 1) == edge, column, turned)

    def tilt(centre, up, down, arrived, i, lines, with_x, with_y):
        stack = []
        for dz in (1, -1):
            r = i if dz > 0 else i + 3

            def row_of(offset):
                return arrived[ZINDEX[offset], r : r + 1, :]

            stack.append(row_of((0, 0, dz)))
            stack.append(
                jnp.where(lane1 < by, row_of((1, 0, dz)), row_of((-1, 0, dz)))
                if with_x
                else jnp.zeros((1, bz), F32)
            )
            stack.append(
                jnp.where(lane1 % by == 0, row_of((0, 1, dz)), row_of((0, -1, dz)))
                if with_y
                else jnp.zeros((1, bz), F32)
            )
        stack = stack + [jnp.zeros((2, bz), F32)]
        columns = jnp.concatenate(stack, axis=0).T
        cells = centre[own, rows, :].reshape(bx * by, bz)
        for dz, out, k in ((1, up, 0), (-1, down, 3)):
            moved = shifted(cells, dz, columns[:, k : k + 1])
            out[own, rows, :] = moved.reshape(bx, by, bz)
            if with_x:
                out[0, rows, :] = shifted(
                    centre[0, rows, :], dz, columns[hi_x * by : bx * by, k + 1 : k + 2]
                )
                out[bx + 1, rows, :] = shifted(
                    centre[bx + 1, rows, :], dz, columns[0:by, k + 1 : k + 2]
                )
            if with_y:
                for side, at, inner in ((0, TOP - 1, hi_y), (1, TOP + by, 0)):
                    edge = jnp.concatenate(
                        [
                            columns[x * by + inner : x * by + inner + 1, k + 2 : k + 3]
                            for x in range(bx)
                        ],
                        axis=0,
                    )
                    moved = shifted(lines[side], dz, edge)
                    for x in range(bx):
                        out[1 + x, at : at + 1, :] = moved[x : x + 1, :]

    for side in range(2):
        for i, slot in enumerate((XY, YY, YZ)):
            lines_in(tens.at[slot], t_yr.at[side, i], side)
    corners_in(tens.at[XY], t_xyr)
    for slot, with_x, with_y in ((XZ, True, False), (YZ, False, True), (ZZ, False, False)):
        i = ZSLOT[slot]
        tilt(
            tens.at[slot],
            tens_p.at[i],
            tens_m.at[i],
            t_zr,
            i,
            (t_yr[0, 2], t_yr[1, 2]),
            with_x,
            with_y,
        )

    def weigh(t, x):
        dx, dy, dz, slot, factor = TAPS[t]
        here = tens[slot, 1 + x, rows, :]
        there_rows = slice(TOP + dy, TOP + dy + by)
        if dz:
            beside = tens_p if dz > 0 else tens_m
            there = beside[ZSLOT[slot], 1 + x + dx, there_rows, :]
        else:
            there = tens[slot, 1 + x + dx, there_rows, :]
        weight[t, x] = factor * (here + there)

    gathered(gat1, 0)
    for d in range(count):
        den1[d * zblk : (d + 1) * zblk, :] = gat1[d]
    every = den1[...]
    lane_b = iota(every.shape, 1)
    number = every[:, COARSE + 2 : COARSE + 3]
    hot = (lane_b.astype(F32) == number).astype(F32)
    rhs = jnp.sum(every[:, COARSE + 1 : COARSE + 2] * hot, axis=0, keepdims=True)
    parts = jnp.where(lane_b <= COARSE, every, 0.0)
    flow = lax.dot_general(
        hot, parts, (((0,), (0,)), ((), ())), precision=HIGHEST, preferred_element_type=F32
    )
    back = lax.dot_general(
        parts, hot, (((0,), (0,)), ((), ())), precision=HIGHEST, preferred_element_type=F32
    )
    flow, back = flow[0:COARSE], back[0:COARSE]
    row_c, lane_c = iota((COARSE, LANES), 0), iota((COARSE, LANES), 1)
    outward = jnp.sum(flow, axis=1, keepdims=True)
    inward = jnp.sum(flow, axis=0, keepdims=True)
    coarse = jnp.where(row_c == lane_c, outward + inward, 0.0) - flow - back
    work = jnp.where(
        lane_c < COARSE,
        (row_c == lane_c).astype(F32),
        pltpu.roll(jnp.where(lane_c < COARSE, coarse, 0.0), COARSE, 1),
    )
    units = [(t, x) for x in range(bx) for t in range(len(TAPS))]
    share = -(-len(units) * PIVOTS // COARSE)
    for k in range(0, COARSE, PIVOTS):
        columns = [
            jnp.broadcast_to(work[:, COARSE + k + c : COARSE + k + c + 1], (COARSE, LANES))
            for c in range(PIVOTS)
        ]
        lines = [work[k + i : k + i + 1, :] for i in range(PIVOTS)]
        pivot = [[columns[c][k + i : k + i + 1, :] for c in range(PIVOTS)] for i in range(PIVOTS)]
        for unit in units[:share]:
            weigh(*unit)
        units = units[share:]
        for i in range(PIVOTS):
            scale = 1.0 / pivot[i][i]
            lines[i] = lines[i] * scale
            for c in range(i + 1, PIVOTS):
                pivot[i][c] = pivot[i][c] * scale
            for r in range(PIVOTS):
                if r != i:
                    ratio = pivot[r][i]
                    lines[r] = lines[r] - ratio * lines[i]
                    for c in range(i + 1, PIVOTS):
                        pivot[r][c] = pivot[r][c] - ratio * pivot[i][c]
        for c in range(PIVOTS):
            work = work - columns[c] * lines[c]
        for i in range(PIVOTS):
            work = jnp.where(row_c == k + i, lines[i], work)
    for unit in units:
        weigh(*unit)
    inverse[0:COARSE, :] = jnp.where(lane_c < COARSE, work, 0.0)
    inverse[COARSE:LANES, :] = jnp.zeros((LANES - COARSE, LANES), F32)

    reach = [
        jnp.dot(near, inverse[...], precision=HIGHEST, preferred_element_type=F32)
        for near in around
    ]

    def solve(row):
        wide = jnp.broadcast_to(row, (8, LANES))
        got = jnp.dot(wide, inverse[...], precision=HIGHEST, preferred_element_type=F32)
        return got[0:1]

    row16, lane16 = iota((16, LANES), 0), iota((16, LANES), 1)
    place16, block16 = lane16 % span, lane16 // span

    def steps(row):
        flat_rows = jnp.zeros((16, LANES), F32)
        up_rows, down_rows = flat_rows, flat_rows
        for j in range(zblk):
            u = jnp.sum(reach[j] * row, axis=1, keepdims=True)
            mine = block16 == j
            flat_rows = jnp.where(mine, u[16:32], flat_rows)
            up_rows = jnp.where(mine, jnp.where(place16 == span - 1, u[32:48], u[16:32]), up_rows)
            down_rows = jnp.where(mine, jnp.where(place16 == 0, u[0:16], u[16:32]), down_rows)
        centre = flat_rows[4:5]
        return centre, {0: centre - flat_rows, 1: centre - up_rows, -1: centre - down_rows}

    plane_row = iota((by, bz), 0)

    def coarse_image(diffs, x):
        total = jnp.zeros((by, bz), F32)
        for t, (dx, dy, dz, _, _) in enumerate(TAPS):
            ax = 1 if x + dx >= bx else (-1 if x + dx < 0 else 0)

            def line(ay):
                r = (ax + 1) * 3 + ay + 1
                return diffs[dz][r : r + 1]

            if dz == 0 and ax == 0 and dy == 0:
                continue
            if dy == 0:
                delta = jnp.broadcast_to(line(0), (by, bz))
            else:
                delta = jnp.where(
                    plane_row == (hi_y if dy > 0 else 0), line(dy), line(0)
                )
            total = total + weight[t, x] * delta
        return total

    index_f = iota((bx * by, LANES), 0)
    same_f = index_f == iota((bx * by, LANES), 1)

    def begin_field(e):
        cells = field[e, own, rows, :].reshape(bx * by, bz)
        for r, at in ((0, 0), (3, bz - 1)):
            column = jnp.where(same_f, cells[:, at : at + 1], 0.0)
            f_zpack[e, r : r + 1, :] = jnp.sum(column, axis=0, keepdims=True)
        for side, y in ((0, 0), (1, hi_y)):
            for x in range(bx):
                f_ypack[e, side, x : x + 1, :] = field[e, 1 + x, TOP + y : TOP + y + 1, :]
        begin, finish = exchange(1 + e, field_ends(e))
        begin()
        return finish

    def operate(e):
        base = field.at[e]
        for side in range(2):
            lines_in(base, f_yr.at[e, side], side)
        corners_in(base, f_xyr.at[e])
        tilt(
            base, field_p, field_m, f_zr.at[e], 0, (f_yr[e, 0], f_yr[e, 1]), True, True
        )
        norm = jnp.zeros((by, bz), F32)
        cross, total = norm, norm
        for x in range(bx):
            here = base[1 + x, rows, :]
            acc = jnp.zeros((by, bz), F32)
            for t, (dx, dy, dz, _, _) in enumerate(TAPS):
                source = base if dz == 0 else (field_p if dz > 0 else field_m)
                there = source[1 + x + dx, TOP + dy : TOP + dy + by, :]
                acc = acc + weight[t, x] * (here - there)
            prod[x] = acc
            norm = norm + here * here
            cross = cross + here * acc
            total = total + acc
        total = jnp.sum(total, axis=0, keepdims=True)
        lists = [jnp.where(block == j, total, 0.0) for j in range(zblk)]
        lists += [jnp.sum(norm, axis=0, keepdims=True), jnp.sum(cross, axis=0, keepdims=True)]
        sums = jnp.sum(jnp.concatenate(lists, axis=0), axis=1, keepdims=True)
        row = jnp.zeros((1, LANES), F32)
        for i, at in enumerate(own_id + [COARSE, COARSE + 1]):
            row = row + jnp.where(lane1 == at, sums[i : i + 1], 0.0)
        msg2[e] = row
        gat2[e, me] = row
        spread(msg2.at[e], gat2.at[e], 1 + e)

    def collect(e):
        gathered(gat2.at[e], 1 + e)
        terms = [gat2[e, d] for d in range(count)]
        while len(terms) > 1:
            pairs = [a + b for a, b in zip(terms[0::2], terms[1::2])]
            terms = pairs + terms[len(pairs) * 2 :]
        row = terms[0]
        values = solve(row)
        shared = jnp.sum(row * values, axis=1, keepdims=True)
        norm = row[:, COARSE : COARSE + 1]
        cross = row[:, COARSE + 1 : COARSE + 2] - shared
        return row, norm, cross

    centre0, diffs = steps(rhs)
    for x in range(bx):
        field[0, 1 + x, rows, :] = right_ref[x] - coarse_image(diffs, x)
    finish = begin_field(0)
    finish()
    operate(0)
    row0, norm0, curve0 = collect(0)
    centre1, diffs = steps(row0)
    alpha0 = norm0 / curve0
    for x in range(bx):
        moved = prod[x] - coarse_image(diffs, x)
        image[x] = moved
        field[1, 1 + x, rows, :] = field[0, 1 + x, rows, :] - alpha0 * moved
    finish = begin_field(1)
    finish()
    operate(1)
    row1, norm1, curve1 = collect(1)
    centre2, diffs = steps(row1)
    beta = norm1 / norm0
    alpha1 = norm1 / (curve1 - beta * norm1 / alpha0)
    both = alpha0 + alpha1 * beta
    coarse_row = centre0 - both * centre1 - alpha1 * centre2
    for x in range(bx):
        moved = prod[x] - coarse_image(diffs, x) + beta * image[x]
        now = field[1, 1 + x, rows, :]
        res_ref[x] = now - alpha1 * moved
        sol_ref[x] = coarse_row + both * field[0, 1 + x, rows, :] + alpha1 * now
    for wait in later:
        wait()


def solution(mesh):
    nx, ny, nz = (mesh.shape[name] for name in ("gx", "gy", "gz"))
    count = nx * ny * nz

    def body(right_side, fiber_class, conductivity_scale, class_tensor, block_ids):
        bx, by, bz = right_side.shape
        nbx, nby, nbz = block_ids.shape
        zblk = nbz // nz
        dims = (nx, ny, nz, bx, by, zblk, nbx, nby, nbz)
        px, py = bx + 2, by + 16
        vmem = lambda *shape: pltpu.VMEM(shape, F32)
        whole = pl.BlockSpec(memory_space=pltpu.VMEM)
        return pl.pallas_call(
            functools.partial(kernel, dims),
            out_shape=[jax.ShapeDtypeStruct((bx, by, bz), F32)] * 2,
            in_specs=[pl.BlockSpec(memory_space=pltpu.HBM)] * 5,
            out_specs=[whole, whole],
            scratch_shapes=[
                pltpu.SMEM(block_ids.shape, jnp.int32),
                pltpu.SMEM(class_tensor.shape, F32),
                vmem(bx, by, bz),
                pltpu.VMEM((bx, by, bz), jnp.int32),
                vmem(bx, by, bz),
                pltpu.SemaphoreType.DMA((5,)),
                vmem(6, px, py, bz),
                vmem(3, px, py, bz),
                vmem(3, px, py, bz),
                vmem(18, bx, by, bz),
                vmem(2, px, py, bz),
                vmem(px, py, bz),
                vmem(px, py, bz),
                vmem(bx, by, bz),
                vmem(bx, by, bz),
                vmem(48, bz),
                vmem(LANES, LANES),
                vmem(2, 3, bx, bz),
                vmem(2, 3, bx, bz),
                vmem(4, bx, bz),
                vmem(8, bz),
                vmem(len(ZOFFSETS), 8, bz),
                vmem(2, 2, bx, bz),
                vmem(2, 2, bx, bz),
                vmem(2, 4, bx, bz),
                vmem(2, 8, bz),
                vmem(2, len(ZOFFSETS), 8, bz),
                vmem(zblk, LANES),
                vmem(count, zblk, LANES),
                vmem(count * zblk, LANES),
                vmem(2, 1, LANES),
                vmem(2, count, 1, LANES),
                pltpu.SemaphoreType.DMA((3, 18)),
                pltpu.SemaphoreType.DMA((3, 18)),
                pltpu.SemaphoreType.DMA((3,)),
                pltpu.SemaphoreType.DMA((3,)),
            ],
            compiler_params=pltpu.CompilerParams(
                collective_id=0, has_side_effects=True
            ),
        )(block_ids, class_tensor, right_side, fiber_class, conductivity_scale)

    placed = (P("gx", "gy", "gz"), P("gx", "gy", "gz"), P("gx", "gy", "gz"), P(), P())
    return jax.shard_map(
        body,
        mesh=mesh,
        in_specs=placed,
        out_specs=(P("gx", "gy", "gz"), P("gx", "gy", "gz")),
        check_vma=False,
    )
```
